32 devices in a mesh: table: 4 (over y, core), dom: 8 (over z, x).
Axes of the slice: x: 2, y: 2, z: 4, core: 2. Of those that a mesh axis runs over, the one named last changes fastest.
Arguments:
- tables: float32 [4, 65536, 128], P('table', 'dom'), may hold values from -6 to 6
- owner_ids: int32 [16384, 4], P(('table', 'dom')), may hold values from 0 to 31, all different within a row; in each aligned block of 512 rows (0 to 511, 512 to 1023, ...) at most 128 rows name the same one
- row_ids: int32 [16384, 4], P(('table', 'dom')), may hold values from 0 to 8191
- neighbour_part: int32 [128, 4], P(('table', 'dom')), may hold values from 0 to 7, all different within a row; in each aligned block of 4 rows (0 to 3, 4 to 7, ...) at most 4 rows name the same one
- neighbour_block: int32 [128, 4], P(('table', 'dom')), may hold values from 0 to 3
- adjacency: bfloat16 [128, 4, 128, 128], P(('table', 'dom')), may hold values from 0.001 to 1.81
- w_in: bfloat16 [128, 1024], replicated, may hold values from -0.5 to 0.5
- w_pool: bfloat16 [1024, 1024], replicated, may hold values from -0.1875 to 0.1875
- w_self: bfloat16 [1024, 1024], replicated, may hold values from -0.1875 to 0.1875
- w_neigh: bfloat16 [1024, 1024], replicated, may hold values from -0.75 to 0.75
- out_gain: bfloat16 [1024], replicated, may hold values from 0.25 to 1.75
- cotangent: bfloat16 [16384, 1024], P(('table', 'dom')), may hold values from -6 to 6
Outputs:
- node_out: bfloat16 [16384, 1024], P(('table', 'dom'))
- table_grad: float32 [4, 65536, 128], P('table', 'dom')
The draws below stay inside these ranges and needn't reach their ends.
Inputs may be any that keep to these rules, and one draw needn't show every extreme that they name: `owner_ids`: the 4 entries of a row differ. Among the 512 rows of one device no owner is named more than 128 times, and in some device's rows some owner is named exactly 128 times. `neighbour_part`: the 4 entries of a row differ. Among the 4 rows of one device no partition is named more than 4 times, and in some device's rows some partition is named exactly 4 times.
All inputs are finite; a program needn't handle non-finite values.
Results may differ from the reference program's by a relative error of at most 0.012.
Values may be sent and summed in bfloat16 or wider, within the bound.
No kernel may reach another device: no remote copies, remote signals or barrier semaphores. Data moves between devices by JAX's collectives and lax.ppermute only.
A program may use at most 128 MiB of HBM per device.

```python
import math
import jax
import jax.numpy as jnp
import numpy as np
from jax import lax

E = 128
H = 1024
TOP = 4
FANOUT = 4
BLOCK = 128
NODE_DEV = 512
ROWS_DEV = 8192
NBLK = 4
ROW_CAP = 128
HALO_CAP = 4
NODES = 16384
TABLES = 4
ROWS = 65536
N_DOM = 8
DEVICES = 32


def shuffled_columns(subkey):
    return jax.random.permutation(subkey, BLOCK)


def draw_adjacency(key, part):
    block_total = NODES // BLOCK
    full_shape = (block_total, FANOUT, BLOCK, BLOCK)
    base_key = jax.random.fold_in(key, 11)
    base_level = jnp.exp(jax.random.uniform(base_key, full_shape, jnp.float32, math.log(0.001), math.log(0.01)))
    ranges = ((0.6, 1.0), (0.2, 0.5), (0.0, 0.3))
    column_ids = jnp.arange(BLOCK, dtype=jnp.int32)
    summed = base_level
    for term_index in range(3):
        lower_end, upper_end = ranges[term_index]
        order_key = jax.random.fold_in(key, 101 + term_index)
        weight_key = jax.random.fold_in(key, 201 + term_index)
        order_keys = jax.random.split(order_key, block_total * FANOUT)
        orders = jax.vmap(shuffled_columns)(order_keys).reshape(block_total, FANOUT, BLOCK).astype(jnp.int32)
        weights = jax.random.uniform(weight_key, (block_total, FANOUT, BLOCK), jnp.float32, lower_end, upper_end)
        summed = summed + weights[..., None] * (orders[..., None] == column_ids).astype(jnp.float32)
    return summed.astype(jnp.bfloat16)


def with_ends(values, rng, smallest, high):
    spot = [jax.random.randint(jax.random.fold_in(rng, axis), (), 0, length) for axis, length in enumerate(values.shape)]
    main_axis = values.shape.index(max(values.shape))
    beside = spot[:main_axis] + [(spot[main_axis] + 1) % values.shape[main_axis]] + spot[main_axis + 1:]
    return values.at[tuple(spot)].set(smallest).at[tuple(beside)].set(high)


def levels(rng, extent, pieces, least, top_value):
    factor_of, own = 1.0, jax.random.fold_in(rng, 6)
    for position, blocks in pieces:
        steps = jnp.exp(jax.random.uniform(jax.random.fold_in(own, position), (blocks,), jnp.float32, least / len(pieces), top_value / len(pieces)))
        factor_of = factor_of * jnp.repeat(steps, extent[position] // blocks).reshape([-1 if axis == position else 1 for axis in range(len(extent))])
    return factor_of


def deal_out(stream_key, own, number, rows, amount, top, reach, skew):
    order = jax.random.permutation(stream_key, amount)
    heavy_load, common = portions_of(amount, rows * top, reach, skew, True), portions_of(amount, rows * top, reach, skew, False)
    places = jnp.arange(amount)

    def named(lengths, offset_by):
        used = int((lengths > 0).sum())
        fixed = max(1, used // 4)
        moved = fixed + (places - fixed + offset_by * (used - fixed)) % max(1, amount - fixed)
        return jnp.zeros((amount,), jnp.int32).at[order[jnp.where(places < fixed, places, moved)]].set(jnp.asarray(lengths, jnp.int32))

    lengths = jnp.where(number % 4 == 0, named(heavy_load, number // 4), named(common, number - number // 4 - 1))
    mixed = jax.random.permutation(jax.random.fold_in(own, 3), amount)
    source_of, receiver = mixed[0:amount // 2 * 2:2], mixed[1:amount // 2 * 2:2]
    room = jnp.minimum(lengths[source_of] - 1, reach - lengths[receiver]) // 2
    room = jnp.where((source_of == order[0]) | (receiver == order[0]) | (lengths[receiver] == 0), 0, jnp.maximum(room, 0))
    moved = jax.random.randint(jax.random.fold_in(own, 4), (amount // 2,), 0, 1 << 20) % (room + 1)
    lengths = lengths.at[source_of].add(-moved).at[receiver].add(moved)
    members = jnp.searchsorted(jnp.cumsum(lengths), jnp.arange(rows * top), side="right").astype(jnp.int32)
    table = members.reshape(top, rows).T
    table = table[jax.random.permutation(jax.random.fold_in(own, 1), rows)]
    offset_by = jax.random.randint(jax.random.fold_in(own, 2), (rows, 1), 0, top)
    return jnp.take_along_axis(table, (jnp.arange(top)[None, :] + offset_by) % top, axis=1)


def portions_of(number_of, total, limit, lean, full):
    loads = [(1 << 20) // math.isqrt(grade ** lean) + 1 for grade in range(1, number_of + 1)]
    largest = limit if full else min(limit, max(-(-total // number_of), total * loads[0] // sum(loads)))
    least = 1 if total - largest >= number_of - 1 else 0
    given, rest = [largest] + [least] * (number_of - 1), total - largest - least * (number_of - 1)
    while rest > 0:
        candidates = [i for i in range(1, number_of) if given[i] < largest] or [i for i in range(1, number_of) if given[i] < limit]
        whole, budget = sum([loads[i] for i in candidates]), rest
        for i in candidates:
            addition = min(limit - given[i], max(1, budget * loads[i] // whole), rest)
            given[i] = given[i] + addition
            rest = rest - addition
    return np.array(given)


def bell_draw(rng, shape, width, most, pieces=(), held_as=jnp.bfloat16):
    entries = width * jax.random.normal(rng, shape, jnp.float32)
    if pieces:
        entries = entries * levels(rng, shape, pieces, -0.22, 0.18)
    return jnp.clip(entries, -most, most).astype(held_as)


def setup_inputs(seed: int = 0) -> dict:
    streams_of = jax.random.split(jax.random.key(seed), 13)
    tables = bell_draw(streams_of[0], (TABLES, ROWS, E), 1.0, 6.0, ((0, 4), (1, 8)), jnp.float32)
    owner_ids_keys = jax.random.split(jax.random.fold_in(streams_of[1], 1), NODES // NODE_DEV)
    owner_ids_turns = jax.random.permutation(jax.random.fold_in(streams_of[1], 3), NODES // NODE_DEV)
    owner_ids = jax.vmap(lambda own, number: deal_out(jax.random.fold_in(streams_of[1], 2), own, number, NODE_DEV, DEVICES, TOP, ROW_CAP, 2))(owner_ids_keys, owner_ids_turns).reshape((NODES, TOP))
    row_ids = with_ends(jax.random.randint(streams_of[2], (NODES, TOP), 0, ROWS_DEV), jax.random.fold_in(streams_of[2], 1), 0, ROWS_DEV - 1).astype(jnp.int32)
    neighbour_part_keys = jax.random.split(jax.random.fold_in(streams_of[3], 1), (NODES // BLOCK) // NBLK)
    neighbour_part_turns = jax.random.permutation(jax.random.fold_in(streams_of[3], 3), (NODES // BLOCK) // NBLK)
    neighbour_part = jax.vmap(lambda own, number: deal_out(jax.random.fold_in(streams_of[3], 2), own, number, NBLK, N_DOM, FANOUT, HALO_CAP, 1))(neighbour_part_keys, neighbour_part_turns).reshape((NODES // BLOCK, FANOUT))
    neighbour_block = with_ends(jax.random.randint(streams_of[4], (NODES // BLOCK, FANOUT), 0, NBLK), jax.random.fold_in(streams_of[4], 1), 0, NBLK - 1).astype(jnp.int32)
    adjacency = draw_adjacency(jax.random.fold_in(streams_of[12], 71), 0)
    w_in = bell_draw(streams_of[6], (E, H), E ** -0.5, 0.5)
    w_pool = bell_draw(streams_of[7], (H, H), H ** -0.5, 0.1875)
    w_self = bell_draw(streams_of[8], (H, H), H ** -0.5, 0.1875)
    w_neigh = bell_draw(streams_of[9], (H, H), (H // 16) ** -0.5, 0.75)
    out_gain = jnp.clip(1.0 + 0.15 * jax.random.normal(streams_of[10], (H,), jnp.float32), 0.25, 1.75).astype(jnp.bfloat16)
    cotangent = bell_draw(streams_of[11], (NODES, H), 1.0, 6.0, ((0, 32),))
    return {"tables": tables, "owner_ids": owner_ids, "row_ids": row_ids, "neighbour_part": neighbour_part, "neighbour_block": neighbour_block, "adjacency": adjacency, "w_in": w_in, "w_pool": w_pool, "w_self": w_self, "w_neigh": w_neigh, "out_gain": out_gain, "cotangent": cotangent}


EPSILON = 1e-06

def silu_slope(inputs):
    sigmoid_part = jax.nn.sigmoid(inputs)
    return sigmoid_part * (1.0 + inputs * (1.0 - sigmoid_part))

def rounded(inputs):
    return lax.optimization_barrier(inputs.astype(jnp.bfloat16)).astype(jnp.float32)

def reference(tables, owner_ids, row_ids, neighbour_part, neighbour_block, adjacency, w_in, w_pool, w_self, w_neigh, out_gain, cotangent):
    table_group = (owner_ids // N_DOM).astype(jnp.int32)
    global_rows = (owner_ids % N_DOM * ROWS_DEV + row_ids).astype(jnp.int32)
    looked = tables[table_group, global_rows]
    feature = lax.optimization_barrier(jnp.sum(looked, axis=1))
    hidden = jnp.dot(feature.astype(jnp.bfloat16), w_in, preferred_element_type=jnp.float32).astype(jnp.bfloat16)
    pooled_pre = jnp.dot(hidden, w_pool, preferred_element_type=jnp.float32)
    pooled = jax.nn.silu(pooled_pre).astype(jnp.bfloat16)
    total_blocks = NODES // BLOCK
    group_blocks = N_DOM * NBLK
    home = jnp.arange(total_blocks, dtype=jnp.int32) // group_blocks
    source_index = (home[:, None] * group_blocks + neighbour_part * NBLK + neighbour_block).astype(jnp.int32)
    pooled_blocks = pooled.reshape(total_blocks, BLOCK, H)
    adj_wide = adjacency.astype(jnp.float32)
    inverse = 1.0 / lax.optimization_barrier(jnp.sum(adj_wide, axis=(1, 3)))
    summed = jnp.zeros((total_blocks, BLOCK, H), jnp.float32)
    for column in range(FANOUT):
        picked = pooled_blocks[source_index[:, column]].astype(jnp.float32)
        summed = summed + jnp.einsum('bij,bjh->bih', adj_wide[:, column], picked, precision=lax.Precision.HIGHEST)
    neighbour_mean = (summed * inverse[:, :, None]).astype(jnp.bfloat16).reshape(NODES, H)
    pre_act = jnp.dot(hidden, w_self, preferred_element_type=jnp.float32) + jnp.dot(neighbour_mean, w_neigh, preferred_element_type=jnp.float32)
    active = jax.nn.silu(pre_act)
    rms_scale = lax.rsqrt(lax.optimization_barrier(jnp.mean(active * active, axis=1, keepdims=True)) + EPSILON)
    gain_wide = out_gain.astype(jnp.float32)
    node_out = (active * rms_scale * gain_wide).astype(jnp.bfloat16)
    weighted = gain_wide * cotangent.astype(jnp.float32)
    d_active = rms_scale * weighted - active * (rms_scale * rms_scale * rms_scale) * lax.optimization_barrier(jnp.mean(weighted * active, axis=1, keepdims=True))
    d_pre = (d_active * silu_slope(pre_act)).astype(jnp.bfloat16)
    d_hidden_self = jnp.dot(d_pre, w_self.T, preferred_element_type=jnp.float32)
    d_mean = jnp.dot(d_pre, w_neigh.T, preferred_element_type=jnp.float32)
    d_scaled = rounded(d_mean.reshape(total_blocks, BLOCK, H) * inverse[:, :, None])
    d_pooled = jnp.zeros((total_blocks, BLOCK, H), jnp.float32)
    for column in range(FANOUT):
        share = rounded(jnp.einsum('bij,bih->bjh', adj_wide[:, column], d_scaled, precision=lax.Precision.HIGHEST))
        d_pooled = d_pooled.at[source_index[:, column]].add(share)
    d_pool_pre = (d_pooled.reshape(NODES, H) * silu_slope(pooled_pre)).astype(jnp.bfloat16)
    d_hidden = (d_hidden_self + jnp.dot(d_pool_pre, w_pool.T, preferred_element_type=jnp.float32)).astype(jnp.bfloat16)
    d_feature = jnp.dot(d_hidden, w_in.T, preferred_element_type=jnp.float32)
    spread = jnp.broadcast_to(d_feature[:, None, :], (NODES, TOP, E))
    table_grad = jnp.zeros((TABLES, ROWS, E), jnp.float32).at[table_group, global_rows].add(spread)
    return (node_out, table_grad)
```

```python
import jax
import jax.numpy as jnp
from jax import lax
from jax.sharding import PartitionSpec as P

EPSILON = 1e-06


def silu_slope(inputs):
    sigmoid_part = jax.nn.sigmoid(inputs)
    return sigmoid_part * (1.0 + inputs * (1.0 - sigmoid_part))


def times_transpose(left_side, right_side):
    return lax.dot_general(
        left_side, right_side, (((1,), (1,)), ((), ())), preferred_element_type=jnp.float32
    )


def bucket_slots(target, buckets, capacity):
    onehot = (target[:, None] == jnp.arange(buckets, dtype=jnp.int32)[None, :]).astype(jnp.int32)
    before = jnp.cumsum(onehot, axis=0) - onehot
    position = jnp.sum(before * onehot, axis=1)
    return target * capacity + position


def swap_all(buffer):
    return lax.all_to_all(buffer, ("table", "dom"), split_axis=0, concat_axis=0, tiled=True)


def body(
    tables,
    owner_ids,
    row_ids,
    neighbour_part,
    neighbour_block,
    adjacency,
    w_in,
    w_pool,
    w_self,
    w_neigh,
    out_gain,
    cotangent,
):
    groups = lax.axis_size("table")
    domains = lax.axis_size("dom")
    devices = groups * domains
    node_count, lookup_count = owner_ids.shape
    table_width = tables.shape[2]
    rows_local = tables.shape[1]
    hidden_width = w_self.shape[0]
    block_rows = adjacency.shape[-1]
    block_count = node_count // block_rows
    fanout = neighbour_part.shape[1]
    capacity = max(2, (2 * node_count * lookup_count + devices - 1) // devices)
    slot_count = devices * capacity

    map_pool = jnp.dot(w_in, w_pool, preferred_element_type=jnp.float32).astype(jnp.bfloat16)
    map_self = jnp.dot(w_in, w_self, preferred_element_type=jnp.float32).astype(jnp.bfloat16)

    row_slots = bucket_slots(owner_ids.reshape(-1), devices, capacity)
    requests = jnp.full((slot_count,), -1, jnp.int32).at[row_slots].set(row_ids.reshape(-1))
    incoming = swap_all(requests.reshape(devices, capacity))
    present = incoming >= 0
    safe_rows = jnp.where(present, incoming, 0)
    fetched = jnp.where(present[:, :, None], tables[0][safe_rows], 0.0).astype(jnp.bfloat16)
    returned = swap_all(fetched).reshape(slot_count, table_width)
    slot_ids = jnp.arange(slot_count, dtype=jnp.int32)
    by_node = row_slots.reshape(node_count, lookup_count)
    select = (by_node[:, 0, None] == slot_ids[None, :])
    for lookup in range(1, lookup_count):
        select = select | (by_node[:, lookup, None] == slot_ids[None, :])
    select = select.astype(jnp.bfloat16)
    feature = jnp.dot(select, returned, preferred_element_type=jnp.float32).astype(jnp.bfloat16)

    gathered = lax.all_gather(feature, "dom", axis=0, tiled=True)
    flat_index = neighbour_part.reshape(-1) * block_count + neighbour_block.reshape(-1)
    sources = gathered.reshape(domains * block_count, block_rows, table_width)[flat_index]
    pooled_pre = jnp.dot(
        sources.reshape(-1, table_width), map_pool, preferred_element_type=jnp.float32
    )
    pooled = jax.nn.silu(pooled_pre).astype(jnp.bfloat16)
    pooled = pooled.reshape(block_count, fanout, block_rows, hidden_width)
    inverse = 1.0 / jnp.sum(adjacency.astype(jnp.float32), axis=(1, 3))
    summed = jnp.einsum("bkij,bkjh->bih", adjacency, pooled, preferred_element_type=jnp.float32)
    neighbour_mean = (
        (summed * inverse[:, :, None]).astype(jnp.bfloat16).reshape(node_count, hidden_width)
    )
    pre_act = jnp.dot(feature, map_self, preferred_element_type=jnp.float32) + jnp.dot(
        neighbour_mean, w_neigh, preferred_element_type=jnp.float32
    )
    active = jax.nn.silu(pre_act)
    rms_scale = lax.rsqrt(jnp.mean(active * active, axis=1, keepdims=True) + EPSILON)
    gain_wide = out_gain.astype(jnp.float32)
    node_out = (active * rms_scale * gain_wide).astype(jnp.bfloat16)
    weighted = gain_wide * cotangent.astype(jnp.float32)
    d_active = rms_scale * weighted - active * (rms_scale * rms_scale * rms_scale) * jnp.mean(
        weighted * active, axis=1, keepdims=True
    )
    d_pre = (d_active * silu_slope(pre_act)).astype(jnp.bfloat16)
    d_self = times_transpose(d_pre, map_self)
    d_mean = times_transpose(d_pre, w_neigh)
    d_scaled = (d_mean.reshape(block_count, block_rows, hidden_width) * inverse[:, :, None]).astype(
        jnp.bfloat16
    )
    shares = jnp.einsum(
        "bkij,bih->bkjh", adjacency, d_scaled, preferred_element_type=jnp.float32
    )
    d_pool_pre = (shares.reshape(-1, hidden_width) * silu_slope(pooled_pre)).astype(jnp.bfloat16)
    d_source = times_transpose(d_pool_pre, map_pool)
    owed = jnp.zeros((domains * block_count, block_rows, table_width), jnp.float32)
    owed = owed.at[flat_index].add(d_source.reshape(-1, block_rows, table_width))
    owed = owed.astype(jnp.bfloat16).reshape(domains, node_count, table_width)
    back = lax.all_to_all(owed, "dom", split_axis=0, concat_axis=0, tiled=True)
    d_feature = (d_self + jnp.sum(back.astype(jnp.float32), axis=0)).astype(jnp.bfloat16)

    outgoing_rows = lax.dot_general(
        select, d_feature, (((0,), (0,)), ((), ())), preferred_element_type=jnp.float32
    ).astype(jnp.bfloat16)
    owed_grads = swap_all(outgoing_rows.reshape(devices, capacity, table_width))
    grad_rows = jnp.where(present, incoming, rows_local).reshape(-1)
    table_grad = (
        jnp.zeros((rows_local, table_width), jnp.float32)
        .at[grad_rows]
        .add(owed_grads.reshape(slot_count, table_width).astype(jnp.float32), mode="drop")
    )
    return (node_out, table_grad[None])


def solution(mesh):
    both = P(("table", "dom"), None)
    placed = (
        P("table", "dom", None),
        both,
        both,
        both,
        both,
        P(("table", "dom"), None, None, None),
        P(),
        P(),
        P(),
        P(),
        P(),
        both,
    )
    return jax.shard_map(
        body,
        mesh=mesh,
        in_specs=placed,
        out_specs=(both, P("table", "dom", None)),
        check_vma=False,
    )
```

```python
import jax
import jax.numpy as jnp
from jax import lax
from jax.experimental import pallas as pl
from jax.experimental.pallas import tpu as pltpu
from jax.sharding import PartitionSpec as P

EPSILON = 1e-06
LANES = 128
GROUP = 16

VMEM = pltpu.VMEM
SMEM = pltpu.SMEM


def call(kernel, outs, ins_space, args, scratch=(), flops=0):
    single = not isinstance(outs, (list, tuple))
    out_list = [outs] if single else list(outs)
    result = pl.pallas_call(
        kernel,
        out_shape=out_list,
        in_specs=[pl.BlockSpec(memory_space=space) for space in ins_space],
        out_specs=[pl.BlockSpec(memory_space=VMEM) for _ in out_list],
        scratch_shapes=list(scratch),
        cost_estimate=pl.CostEstimate(flops=flops, transcendentals=0, bytes_accessed=1 << 20),
    )(*args)
    return result[0] if single else result


def dot(left, right, left_dim, right_dim):
    return lax.dot_general(
        left, right, (((left_dim,), (right_dim,)), ((), ())), preferred_element_type=jnp.float32
    )


def ones_where(mask):
    return jnp.where(mask, 1.0, 0.0).astype(jnp.bfloat16)


def route_kernel(owner_ref, row_ref, request_ref, place_ref):
    lookups, nodes = owner_ref.shape
    devices, capacity = request_ref.shape
    owners = lax.broadcasted_iota(jnp.int32, (devices, nodes), 0)
    earlier = ones_where(
        lax.broadcasted_iota(jnp.int32, (nodes, nodes), 0)
        < lax.broadcasted_iota(jnp.int32, (nodes, nodes), 1)
    )
    hits = [owner_ref[j : j + 1, :] == owners for j in range(lookups)]
    before = dot(jnp.concatenate([ones_where(hit) for hit in hits], axis=0), earlier, 1, 0)
    carry = jnp.zeros((devices, 1), jnp.float32)
    place = jnp.zeros((devices, nodes), jnp.float32)
    slots = lax.broadcasted_iota(jnp.int32, (capacity, nodes), 0).astype(jnp.float32)
    high, low, taken = [], [], []
    for j in range(lookups):
        position = before[j * devices : (j + 1) * devices, :] + carry
        carry = carry + jnp.sum(jnp.where(hits[j], 1.0, 0.0), axis=1, keepdims=True)
        place = place + jnp.where(hits[j], position + 1.0, 0.0)
        own = jnp.sum(jnp.where(hits[j], position, 0.0), axis=0, keepdims=True)
        taken.append(ones_where(own == slots))
        row = row_ref[j : j + 1, :] + 1
        upper = (row >> 7).astype(jnp.float32)
        lower = (row & 127).astype(jnp.float32)
        high.append(jnp.where(hits[j], upper, 0.0).astype(jnp.bfloat16))
        low.append(jnp.where(hits[j], lower, 0.0).astype(jnp.bfloat16))
    taken = jnp.concatenate(taken, axis=1)
    request = dot(jnp.concatenate(high, axis=1), taken, 1, 1) * 128.0 + dot(
        jnp.concatenate(low, axis=1), taken, 1, 1
    )
    request_ref[...] = request.astype(jnp.int32)
    place_ref[...] = place.astype(jnp.int32) - 1


def fetch_kernel(id_ref, table_ref, out_ref, rows_ref):
    chunks = out_ref.shape[0] // LANES
    rows_ref[...] = jnp.zeros(rows_ref.shape, jnp.float32)

    def step(chunk, _):
        for group in range(LANES // GROUP):
            base = chunk * LANES + group * GROUP

            @pl.when(id_ref[base] > 0)
            def _():
                for i in range(GROUP):
                    row = jnp.maximum(id_ref[base + i] - 1, 0)
                    rows_ref[pl.ds(group * GROUP + i, 1), :] = table_ref[pl.ds(row, 1), :]

        start = pl.multiple_of(chunk * LANES, LANES)
        out_ref[pl.ds(start, LANES), :] = rows_ref[...].astype(jnp.bfloat16)
        return 0

    lax.fori_loop(0, chunks, step, 0)


def select_rows(place_ref, first, count, capacity):
    nodes = place_ref.shape[1]
    slots = lax.broadcasted_iota(jnp.int32, (capacity, nodes), 0)
    parts = [ones_where(place_ref[o : o + 1, :] == slots) for o in range(first, first + count)]
    return jnp.concatenate(parts, axis=0)


def combine_kernel(place_ref, returned_ref, feature_ref):
    devices = place_ref.shape[0]
    capacity = returned_ref.shape[0] // devices
    count = max(1, 512 // capacity)
    total = None
    for first in range(0, devices, count):
        chosen = select_rows(place_ref, first, count, capacity)
        rows = returned_ref[first * capacity : (first + count) * capacity, :]
        part = dot(rows, chosen, 0, 0)
        total = part if total is None else total + part
    feature_ref[...] = total.T.astype(jnp.bfloat16)


def spread_kernel(place_ref, d_self_ref, back_ref, out_ref):
    devices = place_ref.shape[0]
    capacity = out_ref.shape[0] // devices
    count = max(1, 512 // capacity)
    total = d_self_ref[...]
    for source in range(back_ref.shape[0]):
        total = total + back_ref[source].astype(jnp.float32)
    d_feature = total.astype(jnp.bfloat16)
    for first in range(0, devices, count):
        chosen = select_rows(place_ref, first, count, capacity)
        out_ref[first * capacity : (first + count) * capacity, :] = dot(
            chosen, d_feature, 1, 0
        ).astype(jnp.bfloat16)


def deposit_kernel(id_ref, ids_ref, grad_ref, out_ref, sums_ref):
    chunks = ids_ref.shape[0]

    def clear(i, _):
        start = pl.multiple_of(i * 256, 256)
        out_ref[pl.ds(start, 256), :] = jnp.zeros((256, out_ref.shape[1]), jnp.float32)
        return 0

    lax.fori_loop(0, out_ref.shape[0] // 256, clear, 0)
    rows = jnp.maximum(ids_ref[...] - 1, 0).astype(jnp.float32)
    columns = rows.T
    same_group = (
        lax.broadcasted_iota(jnp.int32, (LANES, LANES), 0) // GROUP
        == lax.broadcasted_iota(jnp.int32, (LANES, LANES), 1) // GROUP
    )
    for chunk in range(chunks):
        same = (columns[:, chunk : chunk + 1] == rows[chunk : chunk + 1, :]) & same_group
        sums_ref[chunk * LANES : (chunk + 1) * LANES, :] = dot(
            ones_where(same), grad_ref[chunk * LANES : (chunk + 1) * LANES, :], 1, 0
        )

    def step(chunk, _):
        for group in range(LANES // GROUP):
            base = chunk * LANES + group * GROUP

            @pl.when(id_ref[base] > 0)
            def _():
                targets = [jnp.maximum(id_ref[base + i] - 1, 0) for i in range(GROUP)]
                fresh = [
                    out_ref[pl.ds(targets[i], 1), :] + sums_ref[pl.ds(base + i, 1), :]
                    for i in range(GROUP)
                ]
                for i in range(GROUP):
                    out_ref[pl.ds(targets[i], 1), :] = fresh[i]

        return 0

    lax.fori_loop(0, chunks, step, 0)


def sage_kernel(
    index_ref,
    gathered_ref,
    feature_ref,
    adjacency_ref,
    map_pool_ref,
    map_self_ref,
    w_neigh_ref,
    gain_ref,
    cotangent_ref,
    node_out_ref,
    d_self_ref,
    owed_ref,
    slope_ref,
    mean_ref,
    inverse_ref,
    pre_ref,
    d_pre_ref,
    d_mean_ref,
    total_ref,
):
    blocks, fanout, block_rows, _ = adjacency_ref.shape
    nodes, hidden = pre_ref.shape
    span = fanout * block_rows

    def wide(block):
        return jnp.concatenate([adjacency_ref[block, k] for k in range(fanout)], axis=1)

    def forward(block, _):
        sources = jnp.concatenate(
            [gathered_ref[index_ref[block * fanout + k]] for k in range(fanout)], axis=0
        )
        start = pl.multiple_of(block * span, span)
        pooled_pre = dot(sources, map_pool_ref[...], 1, 0)
        gate = 1.0 / (1.0 + jnp.exp(-pooled_pre))
        pooled = (pooled_pre * gate).astype(jnp.bfloat16)
        slope_ref[pl.ds(start, span), :] = gate * (1.0 + pooled_pre * (1.0 - gate))
        weights = wide(block)
        inverse = 1.0 / jnp.sum(weights.astype(jnp.float32), axis=1, keepdims=True)
        own = pl.multiple_of(block * block_rows, block_rows)
        inverse_ref[pl.ds(own, block_rows), :] = jnp.broadcast_to(inverse, (block_rows, LANES))
        mean_ref[pl.ds(own, block_rows), :] = (dot(weights, pooled, 1, 0) * inverse).astype(
            jnp.bfloat16
        )
        return 0

    lax.fori_loop(0, blocks, forward, 0)
    pre_ref[...] = dot(feature_ref[...], map_self_ref[...], 1, 0) + dot(
        mean_ref[...], w_neigh_ref[...], 1, 0
    )
    gain = gain_ref[...].astype(jnp.float32)
    piece = 64

    def middle(part, _):
        start = pl.multiple_of(part * piece, piece)
        here = pl.ds(start, piece)
        pre_act = pre_ref[here, :]
        gate = 1.0 / (1.0 + jnp.exp(-pre_act))
        active = pre_act * gate
        scale = lax.rsqrt(jnp.mean(active * active, axis=1, keepdims=True) + EPSILON)
        node_out_ref[here, :] = (active * scale * gain).astype(jnp.bfloat16)
        weighted = gain * cotangent_ref[here, :].astype(jnp.float32)
        shift = (scale * scale * scale) * jnp.mean(weighted * active, axis=1, keepdims=True)
        d_active = scale * weighted - active * shift
        d_pre_ref[here, :] = (d_active * (gate * (1.0 + pre_act * (1.0 - gate)))).astype(
            jnp.bfloat16
        )
        return 0

    lax.fori_loop(0, nodes // piece, middle, 0)
    d_pre = d_pre_ref[...]
    d_self_ref[...] = dot(d_pre, map_self_ref[...], 1, 1)
    d_mean_ref[...] = dot(d_pre, w_neigh_ref[...], 1, 1)
    total_ref[...] = jnp.zeros(total_ref.shape, jnp.float32)

    def backward(block, _):
        own = pl.multiple_of(block * block_rows, block_rows)
        inverse = inverse_ref[pl.ds(own, block_rows), :][:, :1]
        d_scaled = (d_mean_ref[pl.ds(own, block_rows), :] * inverse).astype(jnp.bfloat16)
        start = pl.multiple_of(block * span, span)
        share = dot(wide(block), d_scaled, 0, 0)
        d_pool = (share * slope_ref[pl.ds(start, span), :]).astype(jnp.bfloat16)
        d_source = dot(d_pool, map_pool_ref[...], 1, 1)
        for k in range(fanout):
            target = index_ref[block * fanout + k]
            total_ref[target] += d_source[k * block_rows : (k + 1) * block_rows, :]
        return 0

    lax.fori_loop(0, blocks, backward, 0)
    owed_ref[...] = total_ref[...].astype(jnp.bfloat16)


def swap_all(buffer):
    return lax.all_to_all(buffer, ("table", "dom"), split_axis=0, concat_axis=0, tiled=True)


def body(
    tables,
    owner_ids,
    row_ids,
    neighbour_part,
    neighbour_block,
    adjacency,
    w_in,
    w_pool,
    w_self,
    w_neigh,
    out_gain,
    cotangent,
):
    groups = lax.axis_size("table")
    domains = lax.axis_size("dom")
    devices = groups * domains
    node_count, lookup_count = owner_ids.shape
    table_width = tables.shape[2]
    rows_local = tables.shape[1]
    hidden = w_self.shape[0]
    block_rows = adjacency.shape[-1]
    block_count = node_count // block_rows
    fanout = neighbour_part.shape[1]
    capacity = max(2, (2 * node_count * lookup_count + devices - 1) // devices)
    slot_count = devices * capacity
    chunks = slot_count // LANES
    f32, bf16 = jnp.float32, jnp.bfloat16

    map_pool = jnp.dot(w_in, w_pool, preferred_element_type=f32).astype(bf16)
    map_self = jnp.dot(w_in, w_self, preferred_element_type=f32).astype(bf16)

    requests, place = call(
        route_kernel,
        [
            jax.ShapeDtypeStruct((devices, capacity), jnp.int32),
            jax.ShapeDtypeStruct((devices, node_count), jnp.int32),
        ],
        [VMEM, VMEM],
        (owner_ids.T, row_ids.T),
    )
    incoming = swap_all(requests)
    flat_ids = incoming.reshape(-1)
    fetched = call(
        fetch_kernel,
        jax.ShapeDtypeStruct((slot_count, table_width), bf16),
        [SMEM, VMEM],
        (flat_ids, tables[0]),
        scratch=[pltpu.VMEM((LANES, table_width), f32)],
    )
    returned = swap_all(fetched.reshape(devices, capacity, table_width))
    feature = call(
        combine_kernel,
        jax.ShapeDtypeStruct((node_count, table_width), bf16),
        [VMEM, VMEM],
        (place, returned.reshape(slot_count, table_width)),
    )
    gathered = lax.all_to_all(
        jnp.broadcast_to(feature[None], (domains, node_count, table_width)),
        "dom",
        split_axis=0,
        concat_axis=0,
        tiled=True,
    )
    flat_index = neighbour_part.reshape(-1) * block_count + neighbour_block.reshape(-1)
    node_out, d_self, owed = call(
        sage_kernel,
        [
            jax.ShapeDtypeStruct((node_count, hidden), bf16),
            jax.ShapeDtypeStruct((node_count, table_width), f32),
            jax.ShapeDtypeStruct((domains * block_count, block_rows, table_width), bf16),
        ],
        [SMEM] + [VMEM] * 8,
        (
            flat_index,
            gathered.reshape(domains * block_count, block_rows, table_width),
            feature,
            adjacency,
            map_pool,
            map_self,
            w_neigh,
            out_gain.reshape(1, hidden),
            cotangent,
        ),
        scratch=[
            pltpu.VMEM((node_count * fanout, hidden), f32),
            pltpu.VMEM((node_count, hidden), bf16),
            pltpu.VMEM((node_count, LANES), f32),
            pltpu.VMEM((node_count, hidden), f32),
            pltpu.VMEM((node_count, hidden), bf16),
            pltpu.VMEM((node_count, hidden), f32),
            pltpu.VMEM((domains * block_count, block_rows, table_width), f32),
        ],
        flops=5 * 10**9,
    )
    back = lax.all_to_all(
        owed.reshape(domains, node_count, table_width),
        "dom",
        split_axis=0,
        concat_axis=0,
        tiled=True,
    )
    outgoing = call(
        spread_kernel,
        jax.ShapeDtypeStruct((slot_count, table_width), bf16),
        [VMEM, VMEM, VMEM],
        (place, d_self, back),
    )
    owed_rows = swap_all(outgoing.reshape(devices, capacity, table_width))
    table_grad = call(
        deposit_kernel,
        jax.ShapeDtypeStruct((rows_local, table_width), f32),
        [SMEM, VMEM, VMEM],
        (flat_ids, flat_ids.reshape(chunks, LANES), owed_rows.reshape(slot_count, table_width)),
        scratch=[pltpu.VMEM((slot_count, table_width), f32)],
    )
    return (node_out, table_grad[None])


def solution(mesh):
    both = P(("table", "dom"), None)
    placed = (
        P("table", "dom", None),
        both,
        both,
        both,
        both,
        P(("table", "dom"), None, None, None),
        P(),
        P(),
        P(),
        P(),
        P(),
        both,
    )
    return jax.shard_map(
        body,
        mesh=mesh,
        in_specs=placed,
        out_specs=(both, P("table", "dom", None)),
        check_vma=False,
    )
```

```python
from functools import partial

import jax
import jax.numpy as jnp
from jax import lax
from jax.experimental import pallas as pl
from jax.experimental.pallas import tpu as pltpu
from jax.sharding import PartitionSpec as P

EPSILON = 1e-06
LANES = 128
GROUP = 16

VMEM = pltpu.VMEM
SMEM = pltpu.SMEM
CHIP = "chip"


def call(kernel, outs, ins_space, args, scratch=(), flops=0):
    single = not isinstance(outs, (list, tuple))
    out_list = [outs] if single else list(outs)
    args = [
        pltpu.with_memory_space_constraint(arg, VMEM) if space == CHIP else arg
        for space, arg in zip(ins_space, args)
    ]
    result = pl.pallas_call(
        kernel,
        out_shape=out_list,
        in_specs=[pl.BlockSpec(memory_space=VMEM if space == CHIP else space) for space in ins_space],
        out_specs=[pl.BlockSpec(memory_space=VMEM) for _ in out_list],
        scratch_shapes=list(scratch),
        compiler_params=pltpu.CompilerParams(vmem_limit_bytes=40 << 20),
        cost_estimate=pl.CostEstimate(flops=flops, transcendentals=0, bytes_accessed=1 << 20),
    )(*args)
    return result[0] if single else result


def on_chip(shape, dtype):
    return pltpu.VMEM(shape, dtype)


def dot(left, right, left_dim, right_dim):
    return lax.dot_general(
        left, right, (((left_dim,), (right_dim,)), ((), ())), preferred_element_type=jnp.float32
    )


def ones_where(mask):
    return jnp.where(mask, 1.0, 0.0).astype(jnp.bfloat16)


def route_kernel(owner_ref, row_ref, request_ref, place_ref):
    lookups, nodes = owner_ref.shape
    devices, capacity = request_ref.shape
    owners = lax.broadcasted_iota(jnp.int32, (devices, nodes), 0)
    earlier = ones_where(
        lax.broadcasted_iota(jnp.int32, (nodes, nodes), 0)
        < lax.broadcasted_iota(jnp.int32, (nodes, nodes), 1)
    )
    hits = [owner_ref[j : j + 1, :] == owners for j in range(lookups)]
    before = dot(jnp.concatenate([ones_where(hit) for hit in hits], axis=0), earlier, 1, 0)
    carry = jnp.zeros((devices, 1), jnp.float32)
    place = jnp.zeros((devices, nodes), jnp.float32)
    slots = lax.broadcasted_iota(jnp.int32, (capacity, nodes), 0).astype(jnp.float32)
    high, low, taken = [], [], []
    for j in range(lookups):
        position = before[j * devices : (j + 1) * devices, :] + carry
        carry = carry + jnp.sum(jnp.where(hits[j], 1.0, 0.0), axis=1, keepdims=True)
        place = place + jnp.where(hits[j], position + 1.0, 0.0)
        own = jnp.sum(jnp.where(hits[j], position, 0.0), axis=0, keepdims=True)
        taken.append(ones_where(own == slots))
        row = row_ref[j : j + 1, :] + 1
        upper = (row >> 7).astype(jnp.float32)
        lower = (row & 127).astype(jnp.float32)
        high.append(jnp.where(hits[j], upper, 0.0).astype(jnp.bfloat16))
        low.append(jnp.where(hits[j], lower, 0.0).astype(jnp.bfloat16))
    taken = jnp.concatenate(taken, axis=1)
    request = dot(jnp.concatenate(high, axis=1), taken, 1, 1) * 128.0 + dot(
        jnp.concatenate(low, axis=1), taken, 1, 1
    )
    request_ref[...] = request.astype(jnp.int32)
    place_ref[...] = place.astype(jnp.int32) - 1


def fetch_kernel(id_ref, table_ref, out_ref, rows_ref):
    chunks = out_ref.shape[0] // LANES
    rows_ref[...] = jnp.zeros(rows_ref.shape, jnp.float32)

    def step(chunk, _):
        for group in range(LANES // GROUP):
            base = chunk * LANES + group * GROUP

            @pl.when(id_ref[base] > 0)
            def _():
                for i in range(GROUP):
                    row = jnp.maximum(id_ref[base + i] - 1, 0)
                    rows_ref[pl.ds(group * GROUP + i, 1), :] = table_ref[pl.ds(row, 1), :]

        start = pl.multiple_of(chunk * LANES, LANES)
        out_ref[pl.ds(start, LANES), :] = rows_ref[...].astype(jnp.bfloat16)
        return 0

    lax.fori_loop(0, chunks, step, 0)


def select_rows(place_ref, first, count, capacity):
    nodes = place_ref.shape[1]
    slots = lax.broadcasted_iota(jnp.int32, (capacity, nodes), 0)
    parts = [ones_where(place_ref[o : o + 1, :] == slots) for o in range(first, first + count)]
    return jnp.concatenate(parts, axis=0)


def combine_kernel(place_ref, returned_ref, feature_ref):
    devices = place_ref.shape[0]
    capacity = returned_ref.shape[0] // devices
    count = max(1, 512 // capacity)
    total = None
    for first in range(0, devices, count):
        chosen = select_rows(place_ref, first, count, capacity)
        rows = returned_ref[first * capacity : (first + count) * capacity, :]
        part = dot(rows, chosen, 0, 0)
        total = part if total is None else total + part
    feature_ref[...] = total.T.astype(jnp.bfloat16)


def spread_kernel(place_ref, d_self_ref, *refs):
    *back_refs, out_ref = refs
    devices = place_ref.shape[0]
    capacity = out_ref.shape[0] // devices
    count = max(1, 512 // capacity)
    total = d_self_ref[...]
    for back_ref in back_refs:
        total = total + back_ref[...].astype(jnp.float32)
    d_feature = total.astype(jnp.bfloat16)
    for first in range(0, devices, count):
        chosen = select_rows(place_ref, first, count, capacity)
        out_ref[first * capacity : (first + count) * capacity, :] = dot(
            chosen, d_feature, 1, 0
        ).astype(jnp.bfloat16)


def deposit_kernel(id_ref, ids_ref, grad_ref, out_ref, sums_ref):
    chunks = ids_ref.shape[0]

    def clear(i, _):
        start = pl.multiple_of(i * 256, 256)
        out_ref[pl.ds(start, 256), :] = jnp.zeros((256, out_ref.shape[1]), jnp.float32)
        return 0

    lax.fori_loop(0, out_ref.shape[0] // 256, clear, 0)
    rows = jnp.maximum(ids_ref[...] - 1, 0).astype(jnp.float32)
    columns = rows.T
    same_group = (
        lax.broadcasted_iota(jnp.int32, (LANES, LANES), 0) // GROUP
        == lax.broadcasted_iota(jnp.int32, (LANES, LANES), 1) // GROUP
    )
    for chunk in range(chunks):
        same = (columns[:, chunk : chunk + 1] == rows[chunk : chunk + 1, :]) & same_group
        sums_ref[chunk * LANES : (chunk + 1) * LANES, :] = dot(
            ones_where(same), grad_ref[chunk * LANES : (chunk + 1) * LANES, :], 1, 0
        )

    def step(chunk, _):
        for group in range(LANES // GROUP):
            base = chunk * LANES + group * GROUP

            @pl.when(id_ref[base] > 0)
            def _():
                targets = [jnp.maximum(id_ref[base + i] - 1, 0) for i in range(GROUP)]
                fresh = [
                    out_ref[pl.ds(targets[i], 1), :] + sums_ref[pl.ds(base + i, 1), :]
                    for i in range(GROUP)
                ]
                for i in range(GROUP):
                    out_ref[pl.ds(targets[i], 1), :] = fresh[i]

        return 0

    lax.fori_loop(0, chunks, step, 0)


def sage_kernel(domains, *refs):
    index_ref, *piece_refs = refs[: domains + 1]
    adjacency_ref, map_pool_ref, map_self_ref, w_neigh_ref, gain_ref, cotangent_ref = refs[
        domains + 1 : domains + 7
    ]
    node_out_ref, d_self_ref, *owed_refs = refs[domains + 7 : 2 * domains + 9]
    (
        gathered_ref,
        slope_ref,
        mean_ref,
        inverse_ref,
        pre_ref,
        d_pre_ref,
        d_mean_ref,
        total_ref,
    ) = refs[2 * domains + 9 :]
    blocks, fanout, block_rows, _ = adjacency_ref.shape
    for mask in range(domains):
        for block in range(blocks):
            gathered_ref[mask * blocks + block] = piece_refs[mask][
                block * block_rows : (block + 1) * block_rows, :
            ]
    nodes, hidden = pre_ref.shape
    span = fanout * block_rows

    def wide(block):
        return jnp.concatenate([adjacency_ref[block, k] for k in range(fanout)], axis=1)

    def forward(block, _):
        sources = jnp.concatenate(
            [gathered_ref[index_ref[block * fanout + k]] for k in range(fanout)], axis=0
        )
        start = pl.multiple_of(block * span, span)
        pooled_pre = dot(sources, map_pool_ref[...], 1, 0)
        gate = 1.0 / (1.0 + jnp.exp(-pooled_pre))
        pooled = (pooled_pre * gate).astype(jnp.bfloat16)
        slope_ref[pl.ds(start, span), :] = gate * (1.0 + pooled_pre * (1.0 - gate))
        weights = wide(block)
        inverse = 1.0 / jnp.sum(weights.astype(jnp.float32), axis=1, keepdims=True)
        own = pl.multiple_of(block * block_rows, block_rows)
        inverse_ref[pl.ds(own, block_rows), :] = jnp.broadcast_to(inverse, (block_rows, LANES))
        mean_ref[pl.ds(own, block_rows), :] = (dot(weights, pooled, 1, 0) * inverse).astype(
            jnp.bfloat16
        )
        return 0

    lax.fori_loop(0, blocks, forward, 0)
    pre_ref[...] = dot(piece_refs[0][...], map_self_ref[...], 1, 0) + dot(
        mean_ref[...], w_neigh_ref[...], 1, 0
    )
    gain = gain_ref[...].astype(jnp.float32)
    piece = 64

    def middle(part, _):
        start = pl.multiple_of(part * piece, piece)
        here = pl.ds(start, piece)
        pre_act = pre_ref[here, :]
        gate = 1.0 / (1.0 + jnp.exp(-pre_act))
        active = pre_act * gate
        scale = lax.rsqrt(jnp.mean(active * active, axis=1, keepdims=True) + EPSILON)
        node_out_ref[here, :] = (active * scale * gain).astype(jnp.bfloat16)
        weighted = gain * cotangent_ref[here, :].astype(jnp.float32)
        shift = (scale * scale * scale) * jnp.mean(weighted * active, axis=1, keepdims=True)
        d_active = scale * weighted - active * shift
        d_pre_ref[here, :] = (d_active * (gate * (1.0 + pre_act * (1.0 - gate)))).astype(
            jnp.bfloat16
        )
        return 0

    lax.fori_loop(0, nodes // piece, middle, 0)
    d_pre = d_pre_ref[...]
    d_self_ref[...] = dot(d_pre, map_self_ref[...], 1, 1)
    d_mean_ref[...] = dot(d_pre, w_neigh_ref[...], 1, 1)
    total_ref[...] = jnp.zeros(total_ref.shape, jnp.float32)

    def backward(block, _):
        own = pl.multiple_of(block * block_rows, block_rows)
        inverse = inverse_ref[pl.ds(own, block_rows), :][:, :1]
        d_scaled = (d_mean_ref[pl.ds(own, block_rows), :] * inverse).astype(jnp.bfloat16)
        start = pl.multiple_of(block * span, span)
        share = dot(wide(block), d_scaled, 0, 0)
        d_pool = (share * slope_ref[pl.ds(start, span), :]).astype(jnp.bfloat16)
        d_source = dot(d_pool, map_pool_ref[...], 1, 1)
        for k in range(fanout):
            target = index_ref[block * fanout + k]
            total_ref[target] += d_source[k * block_rows : (k + 1) * block_rows, :]
        return 0

    lax.fori_loop(0, blocks, backward, 0)
    for mask in range(domains):
        for block in range(blocks):
            owed_refs[mask][block * block_rows : (block + 1) * block_rows, :] = total_ref[
                mask * blocks + block
            ].astype(jnp.bfloat16)


def shift(piece, mask):
    domains = lax.axis_size("dom")
    return lax.ppermute(piece, "dom", [(i, i ^ mask) for i in range(domains)])


def swap_all(buffer):
    return lax.all_to_all(buffer, ("table", "dom"), split_axis=0, concat_axis=0, tiled=True)


def body(
    tables,
    owner_ids,
    row_ids,
    neighbour_part,
    neighbour_block,
    adjacency,
    w_in,
    w_pool,
    w_self,
    w_neigh,
    out_gain,
    cotangent,
):
    groups = lax.axis_size("table")
    domains = lax.axis_size("dom")
    devices = groups * domains
    node_count, lookup_count = owner_ids.shape
    table_width = tables.shape[2]
    rows_local = tables.shape[1]
    hidden = w_self.shape[0]
    block_rows = adjacency.shape[-1]
    block_count = node_count // block_rows
    fanout = neighbour_part.shape[1]
    capacity = max(2, (2 * node_count * lookup_count + devices - 1) // devices)
    slot_count = devices * capacity
    chunks = slot_count // LANES
    f32, bf16 = jnp.float32, jnp.bfloat16

    map_pool = jnp.dot(w_in, w_pool, preferred_element_type=f32).astype(bf16)
    map_self = jnp.dot(w_in, w_self, preferred_element_type=f32).astype(bf16)

    requests, place = call(
        route_kernel,
        [
            on_chip((devices, capacity), jnp.int32),
            on_chip((devices, node_count), jnp.int32),
        ],
        [VMEM, VMEM],
        (owner_ids.T, row_ids.T),
    )
    incoming = swap_all(requests)
    flat_ids = incoming.reshape(-1)
    fetched = call(
        fetch_kernel,
        on_chip((slot_count, table_width), bf16),
        [SMEM, VMEM],
        (flat_ids, tables[0]),
        scratch=[pltpu.VMEM((LANES, table_width), f32)],
    )
    returned = swap_all(fetched.reshape(devices, capacity, table_width))
    feature = call(
        combine_kernel,
        on_chip((node_count, table_width), bf16),
        [CHIP, CHIP],
        (place, returned.reshape(slot_count, table_width)),
    )
    half = domains // 2
    far = shift(feature, half)
    near = [shift(feature, mask) for mask in range(1, half)]
    pieces = [feature, *near, far, *[shift(far, mask) for mask in range(1, half)]]
    index = ((neighbour_part ^ lax.axis_index("dom")) * block_count + neighbour_block).reshape(-1)
    node_out, d_self, *owed = call(
        partial(sage_kernel, domains),
        [
            jax.ShapeDtypeStruct((node_count, hidden), bf16),
            jax.ShapeDtypeStruct((node_count, table_width), f32),
            *[on_chip((node_count, table_width), bf16) for _ in range(domains)],
        ],
        [SMEM] + [CHIP] * domains + [VMEM, CHIP, CHIP, VMEM, VMEM, VMEM],
        (
            index,
            *pieces,
            adjacency,
            map_pool,
            map_self,
            w_neigh,
            out_gain.reshape(1, hidden),
            cotangent,
        ),
        scratch=[
            pltpu.VMEM((domains * block_count, block_rows, table_width), bf16),
            pltpu.VMEM((node_count * fanout, hidden), f32),
            pltpu.VMEM((node_count, hidden), bf16),
            pltpu.VMEM((node_count, LANES), f32),
            pltpu.VMEM((node_count, hidden), f32),
            pltpu.VMEM((node_count, hidden), bf16),
            pltpu.VMEM((node_count, hidden), f32),
            pltpu.VMEM((domains * block_count, block_rows, table_width), f32),
        ],
        flops=5 * 10**9,
    )
    relayed = [shift(owed[half + mask], mask) for mask in range(1, half)]
    back = [shift(owed[mask], mask) for mask in range(1, half)]
    relay = owed[half].astype(f32)
    for piece in relayed:
        relay = relay + piece.astype(f32)
    back = [owed[0], *back, shift(relay.astype(bf16), half)]
    outgoing = call(
        spread_kernel,
        on_chip((slot_count, table_width), bf16),
        [CHIP, VMEM] + [CHIP] * len(back),
        (place, d_self, *back),
    )
    owed_rows = swap_all(outgoing.reshape(devices, capacity, table_width))
    table_grad = call(
        deposit_kernel,
        jax.ShapeDtypeStruct((rows_local, table_width), f32),
        [SMEM, VMEM, CHIP],
        (flat_ids, flat_ids.reshape(chunks, LANES), owed_rows.reshape(slot_count, table_width)),
        scratch=[pltpu.VMEM((slot_count, table_width), f32)],
    )
    return (node_out, table_grad[None])


def solution(mesh):
    both = P(("table", "dom"), None)
    placed = (
        P("table", "dom", None),
        both,
        both,
        both,
        both,
        P(("table", "dom"), None, None, None),
        P(),
        P(),
        P(),
        P(),
        P(),
        both,
    )
    return jax.shard_map(
        body,
        mesh=mesh,
        in_specs=placed,
        out_specs=(both, P("table", "dom", None)),
        check_vma=False,
    )
```

```python
from functools import partial

import jax
import jax.numpy as jnp
from jax import lax
from jax.experimental import pallas as pl
from jax.experimental.pallas import tpu as pltpu
from jax.sharding import PartitionSpec as P

EPSILON = 1e-06
LANES = 128
GROUP = 16

VMEM = pltpu.VMEM
SMEM = pltpu.SMEM
HBM = pltpu.HBM
CHIP = "chip"
SPARE = 8


def call(kernel, outs, ins_space, args, scratch=(), flops=0, aliases=None):
    args = [
        pltpu.with_memory_space_constraint(arg, VMEM if space == CHIP else HBM)
        if space in (CHIP, HBM)
        else arg
        for space, arg in zip(ins_space, args)
    ]
    return pl.pallas_call(
        kernel,
        out_shape=[out for _, out in outs],
        in_specs=[pl.BlockSpec(memory_space=VMEM if s == CHIP else s) for s in ins_space],
        out_specs=[pl.BlockSpec(memory_space=space) for space, _ in outs],
        scratch_shapes=list(scratch),
        input_output_aliases=aliases or {},
        compiler_params=pltpu.CompilerParams(vmem_limit_bytes=40 << 20),
        cost_estimate=pl.CostEstimate(flops=flops, transcendentals=0, bytes_accessed=1 << 20),
    )(*args)


def on_chip(shape, dtype):
    return VMEM, pltpu.VMEM(shape, dtype)


def in_hbm(shape, dtype, space=VMEM):
    return space, jax.ShapeDtypeStruct(shape, dtype)


def dot(left, right, left_dim, right_dim):
    return lax.dot_general(
        left, right, (((left_dim,), (right_dim,)), ((), ())), preferred_element_type=jnp.float32
    )


def ones_where(mask):
    return jnp.where(mask, 1.0, 0.0).astype(jnp.bfloat16)


def sigmoid(inputs):
    return 0.5 * jnp.tanh(0.5 * inputs) + 0.5


def route_kernel(
    owner_in, row_in, table_ref, request_ref, place_ref, held_ref, owner_ref, row_ref, sems
):
    owner_load = pltpu.make_async_copy(owner_in, owner_ref, sems.at[0])
    row_load = pltpu.make_async_copy(row_in, row_ref, sems.at[1])
    load = pltpu.make_async_copy(
        table_ref, held_ref.at[pl.ds(SPARE, table_ref.shape[0]), :], sems.at[2]
    )
    owner_load.start()
    row_load.start()
    load.start()
    held_ref[:SPARE, :] = jnp.zeros((SPARE, held_ref.shape[1]), jnp.float32)
    lookups, nodes = owner_ref.shape
    devices, capacity = request_ref.shape
    owners = lax.broadcasted_iota(jnp.int32, (devices, nodes), 0)
    earlier = ones_where(
        lax.broadcasted_iota(jnp.int32, (nodes, nodes), 0)
        < lax.broadcasted_iota(jnp.int32, (nodes, nodes), 1)
    )
    owner_load.wait()
    row_load.wait()
    hits = [owner_ref[j : j + 1, :] == owners for j in range(lookups)]
    before = dot(jnp.concatenate([ones_where(hit) for hit in hits], axis=0), earlier, 1, 0)
    carry = jnp.zeros((devices, 1), jnp.float32)
    place = jnp.zeros((devices, nodes), jnp.float32)
    slots = lax.broadcasted_iota(jnp.int32, (capacity, nodes), 0).astype(jnp.float32)
    high, low, taken = [], [], []
    for j in range(lookups):
        position = before[j * devices : (j + 1) * devices, :] + carry
        carry = carry + jnp.sum(jnp.where(hits[j], 1.0, 0.0), axis=1, keepdims=True)
        place = place + jnp.where(hits[j], position + 1.0, 0.0)
        own = jnp.sum(jnp.where(hits[j], position, 0.0), axis=0, keepdims=True)
        taken.append(ones_where(own == slots))
        row = row_ref[j : j + 1, :] + 1
        upper = (row >> 7).astype(jnp.float32)
        lower = (row & 127).astype(jnp.float32)
        high.append(jnp.where(hits[j], upper, 0.0).astype(jnp.bfloat16))
        low.append(jnp.where(hits[j], lower, 0.0).astype(jnp.bfloat16))
    taken = jnp.concatenate(taken, axis=1)
    request = dot(jnp.concatenate(high, axis=1), taken, 1, 1) * 128.0 + dot(
        jnp.concatenate(low, axis=1), taken, 1, 1
    )
    request_ref[...] = request.astype(jnp.int32)
    place_ref[...] = place.astype(jnp.int32) - 1
    load.wait()


def prep_kernel(
    _,
    w_in_ref,
    w_pool_ref,
    w_self_ref,
    map_pool_ref,
    map_self_ref,
    sums_ref,
    w_in_held,
    w_pool_held,
    w_self_held,
    sems,
):
    copies = [
        pltpu.make_async_copy(source, target, sems.at[i])
        for i, (source, target) in enumerate(
            [(w_in_ref, w_in_held), (w_pool_ref, w_pool_held), (w_self_ref, w_self_held)]
        )
    ]
    for copy in copies:
        copy.start()

    def clear(i, _):
        start = pl.multiple_of(i * 64, 64)
        sums_ref[pl.ds(start, 64), :] = jnp.zeros((64, sums_ref.shape[1]), jnp.float32)
        return 0

    whole = sums_ref.shape[0] // 64
    lax.fori_loop(0, whole, clear, 0)
    rest = sums_ref.shape[0] - whole * 64
    if rest:
        sums_ref[whole * 64 :, :] = jnp.zeros((rest, sums_ref.shape[1]), jnp.float32)
    copies[0].wait()
    copies[1].wait()
    map_pool_ref[...] = dot(w_in_held[...], w_pool_held[...], 1, 0).astype(jnp.bfloat16)
    copies[2].wait()
    map_self_ref[...] = dot(w_in_held[...], w_self_held[...], 1, 0).astype(jnp.bfloat16)


def fetch_kernel(id_ref, table_ref, out_ref, rows_ref):
    chunks = out_ref.shape[0] // LANES
    rows_ref[...] = jnp.zeros(rows_ref.shape, jnp.float32)

    def step(chunk, _):
        for group in range(LANES // GROUP):
            base = chunk * LANES + group * GROUP

            @pl.when(id_ref[base] > 0)
            def _():
                for i in range(GROUP):
                    row = id_ref[base + i] + (SPARE - 1)
                    rows_ref[pl.ds(group * GROUP + i, 1), :] = table_ref[pl.ds(row, 1), :]

        start = pl.multiple_of(chunk * LANES, LANES)
        out_ref[pl.ds(start, LANES), :] = rows_ref[...].astype(jnp.bfloat16)
        return 0

    lax.fori_loop(0, chunks, step, 0)


def select_rows(place_ref, first, count, capacity):
    nodes = place_ref.shape[1]
    slots = lax.broadcasted_iota(jnp.int32, (capacity, nodes), 0)
    parts = [ones_where(place_ref[o : o + 1, :] == slots) for o in range(first, first + count)]
    return jnp.concatenate(parts, axis=0)


def combine_kernel(place_ref, returned_ref, _, feature_ref):
    devices = place_ref.shape[0]
    capacity = returned_ref.shape[0] // devices
    count = max(1, 512 // capacity)
    total = None
    for first in range(0, devices, count):
        chosen = select_rows(place_ref, first, count, capacity)
        rows = returned_ref[first * capacity : (first + count) * capacity, :]
        part = dot(rows, chosen, 0, 0)
        total = part if total is None else total + part
    feature_ref[...] = total.T.astype(jnp.bfloat16)


def spread_kernel(place_ref, d_self_ref, *refs):
    *back_refs, out_ref = refs
    devices = place_ref.shape[0]
    capacity = out_ref.shape[0] // devices
    count = max(1, 512 // capacity)
    total = d_self_ref[...]
    for back_ref in back_refs:
        total = total + back_ref[...].astype(jnp.float32)
    d_feature = total.astype(jnp.bfloat16)
    for first in range(0, devices, count):
        chosen = select_rows(place_ref, first, count, capacity)
        out_ref[first * capacity : (first + count) * capacity, :] = dot(
            chosen, d_feature, 1, 0
        ).astype(jnp.bfloat16)


def deposit_kernel(id_ref, ids_ref, grad_ref, _, sums_ref, out_ref, fresh_ref, sem):
    chunks = ids_ref.shape[0]
    rows = ids_ref[...].astype(jnp.float32)
    columns = rows.T
    same_group = (
        lax.broadcasted_iota(jnp.int32, (LANES, LANES), 0) // GROUP
        == lax.broadcasted_iota(jnp.int32, (LANES, LANES), 1) // GROUP
    )
    for chunk in range(chunks):
        same = (columns[:, chunk : chunk + 1] == rows[chunk : chunk + 1, :]) & same_group
        fresh_ref[chunk * LANES : (chunk + 1) * LANES, :] = dot(
            ones_where(same), grad_ref[chunk * LANES : (chunk + 1) * LANES, :], 1, 0
        )

    def step(chunk, _):
        for group in range(LANES // GROUP):
            base = chunk * LANES + group * GROUP

            @pl.when(id_ref[base] > 0)
            def _():
                targets = [id_ref[base + i] + (SPARE - 1) for i in range(GROUP)]
                fresh = [
                    sums_ref[pl.ds(targets[i], 1), :] + fresh_ref[pl.ds(base + i, 1), :]
                    for i in range(GROUP)
                ]
                for i in range(GROUP):
                    sums_ref[pl.ds(targets[i], 1), :] = fresh[i]

        return 0

    lax.fori_loop(0, chunks, step, 0)
    store = pltpu.make_async_copy(sums_ref.at[pl.ds(SPARE, out_ref.shape[0]), :], out_ref, sem)
    store.start()
    store.wait()


def sage_kernel(domains, *refs):
    index_ref, *piece_refs = refs[: domains + 1]
    gain_ref, *in_refs = refs[domains + 1 : domains + 7]
    node_out_ref, d_self_ref, *owed_refs = refs[domains + 7 : 2 * domains + 9]
    (
        map_pool_ref,
        adjacency_ref,
        map_self_ref,
        w_neigh_ref,
        cotangent_ref,
        sems,
        result_ref,
        gathered_ref,
        slope_ref,
        mean_ref,
        inverse_ref,
        pre_ref,
        d_pre_ref,
        d_mean_ref,
        total_ref,
    ) = refs[2 * domains + 9 :]
    blocks, fanout, block_rows, _ = adjacency_ref.shape
    held = [map_pool_ref, adjacency_ref, map_self_ref, w_neigh_ref, cotangent_ref]
    loads = [
        pltpu.make_async_copy(source, target, sems.at[i])
        for i, (source, target) in enumerate(zip(in_refs, held))
    ]
    for load in loads:
        load.start()
    for mask in range(domains):
        for block in range(blocks):
            gathered_ref[mask * blocks + block] = piece_refs[mask][
                block * block_rows : (block + 1) * block_rows, :
            ]
    nodes, hidden = pre_ref.shape
    span = fanout * block_rows

    def wide(block):
        return jnp.concatenate([adjacency_ref[block, k] for k in range(fanout)], axis=1)

    def forward(block, _):
        sources = jnp.concatenate(
            [gathered_ref[index_ref[block * fanout + k]] for k in range(fanout)], axis=0
        )
        start = pl.multiple_of(block * span, span)
        pooled_pre = dot(sources, map_pool_ref[...], 1, 0)
        gate = sigmoid(pooled_pre)
        pooled = (pooled_pre * gate).astype(jnp.bfloat16)
        slope_ref[pl.ds(start, span), :] = gate * (1.0 + pooled_pre * (1.0 - gate))
        weights = wide(block)
        inverse = 1.0 / jnp.sum(weights.astype(jnp.float32), axis=1, keepdims=True)
        own = pl.multiple_of(block * block_rows, block_rows)
        inverse_ref[pl.ds(own, block_rows), :] = jnp.broadcast_to(inverse, (block_rows, LANES))
        mean_ref[pl.ds(own, block_rows), :] = (dot(weights, pooled, 1, 0) * inverse).astype(
            jnp.bfloat16
        )
        return 0

    loads[0].wait()
    loads[1].wait()
    lax.fori_loop(0, blocks, forward, 0)
    for load in loads[2:]:
        load.wait()
    pre_ref[...] = dot(piece_refs[0][...], map_self_ref[...], 1, 0) + dot(
        mean_ref[...], w_neigh_ref[...], 1, 0
    )
    gain = gain_ref[...].astype(jnp.float32)
    piece = 64

    def middle(part, _):
        start = pl.multiple_of(part * piece, piece)
        here = pl.ds(start, piece)
        pre_act = pre_ref[here, :]
        gate = sigmoid(pre_act)
        active = pre_act * gate
        scale = lax.rsqrt(jnp.mean(active * active, axis=1, keepdims=True) + EPSILON)
        result_ref[here, :] = (active * scale * gain).astype(jnp.bfloat16)
        weighted = gain * cotangent_ref[here, :].astype(jnp.float32)
        shift = (scale * scale * scale) * jnp.mean(weighted * active, axis=1, keepdims=True)
        d_active = scale * weighted - active * shift
        d_pre_ref[here, :] = (d_active * (gate * (1.0 + pre_act * (1.0 - gate)))).astype(
            jnp.bfloat16
        )
        return 0

    lax.fori_loop(0, nodes // piece, middle, 0)
    store = pltpu.make_async_copy(result_ref, node_out_ref, sems.at[len(loads)])
    store.start()
    d_pre = d_pre_ref[...]
    d_self_ref[...] = dot(d_pre, map_self_ref[...], 1, 1)
    d_mean_ref[...] = dot(d_pre, w_neigh_ref[...], 1, 1)
    total_ref[...] = jnp.zeros(total_ref.shape, jnp.float32)

    def backward(block, _):
        own = pl.multiple_of(block * block_rows, block_rows)
        inverse = inverse_ref[pl.ds(own, block_rows), :][:, :1]
        d_scaled = (d_mean_ref[pl.ds(own, block_rows), :] * inverse).astype(jnp.bfloat16)
        start = pl.multiple_of(block * span, span)
        share = dot(wide(block), d_scaled, 0, 0)
        d_pool = (share * slope_ref[pl.ds(start, span), :]).astype(jnp.bfloat16)
        d_source = dot(d_pool, map_pool_ref[...], 1, 1)
        for k in range(fanout):
            target = index_ref[block * fanout + k]
            total_ref[target] += d_source[k * block_rows : (k + 1) * block_rows, :]
        return 0

    lax.fori_loop(0, blocks, backward, 0)
    for mask in range(domains):
        for block in range(blocks):
            owed_refs[mask][block * block_rows : (block + 1) * block_rows, :] = total_ref[
                mask * blocks + block
            ].astype(jnp.bfloat16)
    store.wait()


def shift(piece, mask):
    domains = lax.axis_size("dom")
    return lax.ppermute(piece, "dom", [(i, i ^ mask) for i in range(domains)])


def swap_all(buffer):
    return lax.all_to_all(buffer, ("table", "dom"), split_axis=0, concat_axis=0, tiled=True)


def body(
    tables,
    owner_ids,
    row_ids,
    neighbour_part,
    neighbour_block,
    adjacency,
    w_in,
    w_pool,
    w_self,
    w_neigh,
    out_gain,
    cotangent,
):
    groups = lax.axis_size("table")
    domains = lax.axis_size("dom")
    devices = groups * domains
    node_count, lookup_count = owner_ids.shape
    table_width = tables.shape[2]
    rows_local = tables.shape[1]
    hidden = w_self.shape[0]
    block_rows = adjacency.shape[-1]
    block_count = node_count // block_rows
    fanout = neighbour_part.shape[1]
    capacity = max(2, (2 * node_count * lookup_count + devices - 1) // devices)
    slot_count = devices * capacity
    chunks = slot_count // LANES
    f32, bf16 = jnp.float32, jnp.bfloat16

    requests, place, held = call(
        route_kernel,
        [
            on_chip((devices, capacity), jnp.int32),
            on_chip((devices, node_count), jnp.int32),
            on_chip((rows_local + SPARE, table_width), f32),
        ],
        [HBM, HBM, HBM],
        (owner_ids.T, row_ids.T, tables[0]),
        scratch=[
            pltpu.VMEM((lookup_count, node_count), jnp.int32),
            pltpu.VMEM((lookup_count, node_count), jnp.int32),
            pltpu.SemaphoreType.DMA((3,)),
        ],
    )
    flat_ids = swap_all(requests).reshape(-1)
    (fetched,) = call(
        fetch_kernel,
        [on_chip((slot_count, table_width), bf16)],
        [SMEM, CHIP],
        (flat_ids, held),
        scratch=[pltpu.VMEM((LANES, table_width), f32)],
    )
    returned = swap_all(fetched.reshape(devices, capacity, table_width))
    map_pool, map_self, cleared = call(
        prep_kernel,
        [
            in_hbm((table_width, hidden), bf16),
            in_hbm((table_width, hidden), bf16),
            on_chip((rows_local + SPARE, table_width), f32),
        ],
        [CHIP] + [HBM] * 3,
        (fetched, w_in, w_pool, w_self),
        scratch=[
            pltpu.VMEM(w_in.shape, bf16),
            pltpu.VMEM(w_pool.shape, bf16),
            pltpu.VMEM(w_self.shape, bf16),
            pltpu.SemaphoreType.DMA((3,)),
        ],
        flops=10**9,
    )
    (feature,) = call(
        combine_kernel,
        [on_chip((node_count, table_width), bf16)],
        [CHIP, CHIP, HBM],
        (place, returned.reshape(slot_count, table_width), map_pool),
    )
    half = domains // 2
    far = shift(feature, half)
    near = [shift(feature, mask) for mask in range(1, half)]
    pieces = [feature, *near, far, *[shift(far, mask) for mask in range(1, half)]]
    index = ((neighbour_part ^ lax.axis_index("dom")) * block_count + neighbour_block).reshape(-1)
    node_out, d_self, *owed = call(
        partial(sage_kernel, domains),
        [
            in_hbm((node_count, hidden), bf16, HBM),
            in_hbm((node_count, table_width), f32),
            *[on_chip((node_count, table_width), bf16) for _ in range(domains)],
        ],
        [SMEM] + [CHIP] * domains + [VMEM] + [HBM] * 5,
        (
            index,
            *pieces,
            out_gain.reshape(1, hidden),
            map_pool,
            adjacency,
            map_self,
            w_neigh,
            cotangent,
        ),
        scratch=[
            pltpu.VMEM(map_pool.shape, bf16),
            pltpu.VMEM(adjacency.shape, bf16),
            pltpu.VMEM(map_self.shape, bf16),
            pltpu.VMEM(w_neigh.shape, bf16),
            pltpu.VMEM(cotangent.shape, bf16),
            pltpu.SemaphoreType.DMA((6,)),
            pltpu.VMEM((node_count, hidden), bf16),
            pltpu.VMEM((domains * block_count, block_rows, table_width), bf16),
            pltpu.VMEM((node_count * fanout, hidden), f32),
            pltpu.VMEM((node_count, hidden), bf16),
            pltpu.VMEM((node_count, LANES), f32),
            pltpu.VMEM((node_count, hidden), f32),
            pltpu.VMEM((node_count, hidden), bf16),
            pltpu.VMEM((node_count, hidden), f32),
            pltpu.VMEM((domains * block_count, block_rows, table_width), f32),
        ],
        flops=5 * 10**9,
    )
    relayed = [shift(owed[half + mask], mask) for mask in range(1, half)]
    back = [shift(owed[mask], mask) for mask in range(1, half)]
    relay = owed[half].astype(f32)
    for piece in relayed:
        relay = relay + piece.astype(f32)
    back = [owed[0], *back, shift(relay.astype(bf16), half)]
    (outgoing,) = call(
        spread_kernel,
        [on_chip((slot_count, table_width), bf16)],
        [CHIP, VMEM] + [CHIP] * len(back),
        (place, d_self, *back),
    )
    owed_rows = swap_all(outgoing.reshape(devices, capacity, table_width))
    _, table_grad = call(
        deposit_kernel,
        [
            on_chip((rows_local + SPARE, table_width), f32),
            in_hbm((rows_local, table_width), f32, HBM),
        ],
        [SMEM, VMEM, CHIP, CHIP],
        (
            flat_ids,
            flat_ids.reshape(chunks, LANES),
            owed_rows.reshape(slot_count, table_width),
            cleared,
        ),
        scratch=[pltpu.VMEM((slot_count, table_width), f32), pltpu.SemaphoreType.DMA],
        aliases={3: 0},
    )
    return (node_out, table_grad[None])


def solution(mesh):
    both = P(("table", "dom"), None)
    placed = (
        P("table", "dom", None),
        both,
        both,
        both,
        both,
        P(("table", "dom"), None, None, None),
        P(),
        P(),
        P(),
        P(),
        P(),
        both,
    )
    return jax.shard_map(
        body,
        mesh=mesh,
        in_specs=placed,
        out_specs=(both, P("table", "dom", None)),
        check_vma=False,
    )
```

```python
from functools import partial

import jax
import jax.numpy as jnp
from jax import lax
from jax.experimental import pallas as pl
from jax.experimental.pallas import tpu as pltpu
from jax.sharding import PartitionSpec as P

EPSILON = 1e-06
LANES = 128

VMEM = pltpu.VMEM
SMEM = pltpu.SMEM
HBM = pltpu.HBM
CHIP = "chip"
SPARE = 8


def call(kernel, outs, ins_space, args, scratch=(), flops=0, aliases=None):
    args = [
        pltpu.with_memory_space_constraint(arg, VMEM if space == CHIP else HBM)
        if space in (CHIP, HBM)
        else arg
        for space, arg in zip(ins_space, args)
    ]
    return pl.pallas_call(
        kernel,
        out_shape=[out for _, out in outs],
        in_specs=[pl.BlockSpec(memory_space=VMEM if s == CHIP else s) for s in ins_space],
        out_specs=[pl.BlockSpec(memory_space=space) for space, _ in outs],
        scratch_shapes=list(scratch),
        input_output_aliases=aliases or {},
        compiler_params=pltpu.CompilerParams(vmem_limit_bytes=40 << 20),
        cost_estimate=pl.CostEstimate(flops=flops, transcendentals=0, bytes_accessed=1 << 20),
    )(*args)


def on_chip(shape, dtype):
    return VMEM, pltpu.VMEM(shape, dtype)


def in_hbm(shape, dtype, space=VMEM):
    return space, jax.ShapeDtypeStruct(shape, dtype)


def dot(left, right, left_dim, right_dim):
    return lax.dot_general(
        left, right, (((left_dim,), (right_dim,)), ((), ())), preferred_element_type=jnp.float32
    )


def ones_where(mask):
    return jnp.where(mask, 1.0, 0.0).astype(jnp.bfloat16)


def silu_parts(half):
    upper = jnp.tanh(half) + 1.0
    value = half * upper
    return value, upper + value * (2.0 - upper)


def route_kernel(
    owner_in, row_in, table_ref, request_ref, place_ref, held_ref, owner_ref, row_ref, sems
):
    owner_load = pltpu.make_async_copy(owner_in, owner_ref, sems.at[0])
    row_load = pltpu.make_async_copy(row_in, row_ref, sems.at[1])
    load = pltpu.make_async_copy(
        table_ref, held_ref.at[pl.ds(SPARE, table_ref.shape[0]), :], sems.at[2]
    )
    owner_load.start()
    row_load.start()
    load.start()
    held_ref[:SPARE, :] = jnp.zeros((SPARE, held_ref.shape[1]), jnp.float32)
    lookups, nodes = owner_ref.shape
    devices, capacity = request_ref.shape
    owners = lax.broadcasted_iota(jnp.int32, (devices, nodes), 0)
    earlier = ones_where(
        lax.broadcasted_iota(jnp.int32, (nodes, nodes), 0)
        < lax.broadcasted_iota(jnp.int32, (nodes, nodes), 1)
    )
    owner_load.wait()
    row_load.wait()
    hits = [owner_ref[j : j + 1, :] == owners for j in range(lookups)]
    before = dot(jnp.concatenate([ones_where(hit) for hit in hits], axis=0), earlier, 1, 0)
    carry = jnp.zeros((devices, 1), jnp.float32)
    place = jnp.zeros((devices, nodes), jnp.float32)
    slots = lax.broadcasted_iota(jnp.int32, (capacity, nodes), 0).astype(jnp.float32)
    high, low, taken = [], [], []
    for j in range(lookups):
        position = before[j * devices : (j + 1) * devices, :] + carry
        carry = carry + jnp.sum(jnp.where(hits[j], 1.0, 0.0), axis=1, keepdims=True)
        place = place + jnp.where(hits[j], position + 1.0, 0.0)
        own = jnp.sum(jnp.where(hits[j], position, 0.0), axis=0, keepdims=True)
        taken.append(ones_where(own == slots))
        row = row_ref[j : j + 1, :] + 1
        upper = (row >> 7).astype(jnp.float32)
        lower = (row & 127).astype(jnp.float32)
        high.append(jnp.where(hits[j], upper, 0.0).astype(jnp.bfloat16))
        low.append(jnp.where(hits[j], lower, 0.0).astype(jnp.bfloat16))
    taken = jnp.concatenate(taken, axis=1)
    request = dot(jnp.concatenate(high, axis=1), taken, 1, 1) * 128.0 + dot(
        jnp.concatenate(low, axis=1), taken, 1, 1
    )
    request_ref[...] = request.astype(jnp.int32)
    place_ref[...] = place.astype(jnp.int32) - 1
    load.wait()


def prep_kernel(
    _,
    w_in_ref,
    w_pool_ref,
    w_self_ref,
    map_pool_ref,
    map_self_ref,
    sums_ref,
    w_in_held,
    w_pool_held,
    w_self_held,
    sems,
):
    copies = [
        pltpu.make_async_copy(source, target, sems.at[i])
        for i, (source, target) in enumerate(
            [(w_in_ref, w_in_held), (w_pool_ref, w_pool_held), (w_self_ref, w_self_held)]
        )
    ]
    for copy in copies:
        copy.start()

    def clear(i, _):
        start = pl.multiple_of(i * 64, 64)
        sums_ref[pl.ds(start, 64), :] = jnp.zeros((64, sums_ref.shape[1]), jnp.float32)
        return 0

    whole = sums_ref.shape[0] // 64
    lax.fori_loop(0, whole, clear, 0)
    rest = sums_ref.shape[0] - whole * 64
    if rest:
        sums_ref[whole * 64 :, :] = jnp.zeros((rest, sums_ref.shape[1]), jnp.float32)
    copies[0].wait()
    copies[1].wait()
    map_pool_ref[...] = (0.5 * dot(w_in_held[...], w_pool_held[...], 1, 0)).astype(jnp.bfloat16)
    copies[2].wait()
    map_self_ref[...] = (0.5 * dot(w_in_held[...], w_self_held[...], 1, 0)).astype(jnp.bfloat16)


def fetch_kernel(size, id_ref, table_ref, out_ref, rows_ref):
    chunks = out_ref.shape[0] // LANES
    rows_ref[...] = jnp.zeros(rows_ref.shape, jnp.float32)

    def step(chunk, _):
        for group in range(LANES // size):
            base = chunk * LANES + group * size

            @pl.when(id_ref[base] > 0)
            def _():
                for i in range(size):
                    row = id_ref[base + i] + (SPARE - 1)
                    rows_ref[pl.ds(group * size + i, 1), :] = table_ref[pl.ds(row, 1), :]

        start = pl.multiple_of(chunk * LANES, LANES)
        out_ref[pl.ds(start, LANES), :] = rows_ref[...].astype(jnp.bfloat16)
        return 0

    lax.fori_loop(0, chunks, step, 0)


def select_rows(place_ref, first, count, capacity):
    nodes = place_ref.shape[1]
    slots = lax.broadcasted_iota(jnp.int32, (capacity, nodes), 0)
    parts = [ones_where(place_ref[o : o + 1, :] == slots) for o in range(first, first + count)]
    return jnp.concatenate(parts, axis=0)


def combine_kernel(place_ref, returned_ref, _, feature_ref):
    devices = place_ref.shape[0]
    capacity = returned_ref.shape[0] // devices
    count = max(1, 512 // capacity)
    total = None
    for first in range(0, devices, count):
        chosen = select_rows(place_ref, first, count, capacity)
        rows = returned_ref[first * capacity : (first + count) * capacity, :]
        part = dot(rows, chosen, 0, 0)
        total = part if total is None else total + part
    feature_ref[...] = total.T.astype(jnp.bfloat16)


def spread_kernel(place_ref, d_self_ref, *refs):
    *back_refs, out_ref = refs
    devices = place_ref.shape[0]
    capacity = out_ref.shape[0] // devices
    count = max(1, 512 // capacity)
    total = d_self_ref[...]
    for back_ref in back_refs:
        total = total + back_ref[...].astype(jnp.float32)
    d_feature = total.astype(jnp.bfloat16)
    for first in range(0, devices, count):
        chosen = select_rows(place_ref, first, count, capacity)
        out_ref[first * capacity : (first + count) * capacity, :] = dot(
            chosen, d_feature, 1, 0
        ).astype(jnp.bfloat16)


def deposit_kernel(
    size, gate, id_ref, ids_ref, grad_ref, _, sums_ref, out_ref, fresh_ref, sem
):
    chunks = ids_ref.shape[0]
    rows = ids_ref[...].astype(jnp.float32)
    columns = rows.T
    same_group = (
        lax.broadcasted_iota(jnp.int32, (LANES, LANES), 0) // size
        == lax.broadcasted_iota(jnp.int32, (LANES, LANES), 1) // size
    )
    for chunk in range(chunks):
        same = (columns[:, chunk : chunk + 1] == rows[chunk : chunk + 1, :]) & same_group
        fresh_ref[chunk * LANES : (chunk + 1) * LANES, :] = dot(
            ones_where(same), grad_ref[chunk * LANES : (chunk + 1) * LANES, :], 1, 0
        )

    def step(chunk, _):
        for part in range(LANES // gate):
            first = chunk * LANES + part * gate

            @pl.when(id_ref[first] > 0)
            def _():
                for group in range(gate // size):
                    base = first + group * size
                    targets = [id_ref[base + i] + (SPARE - 1) for i in range(size)]
                    fresh = [
                        sums_ref[pl.ds(targets[i], 1), :] + fresh_ref[pl.ds(base + i, 1), :]
                        for i in range(size)
                    ]
                    for i in range(size):
                        sums_ref[pl.ds(targets[i], 1), :] = fresh[i]

        return 0

    lax.fori_loop(0, chunks, step, 0)
    store = pltpu.make_async_copy(sums_ref.at[pl.ds(SPARE, out_ref.shape[0]), :], out_ref, sem)
    store.start()
    store.wait()


def sage_kernel(domains, *refs):
    index_in, *piece_refs = refs[: domains + 1]
    in_refs = refs[domains + 1 : domains + 7]
    node_out_ref, d_self_ref, *owed_refs = refs[domains + 7 : 2 * domains + 9]
    (
        map_pool_ref,
        adjacency_ref,
        map_self_ref,
        w_neigh_ref,
        gain_ref,
        cotangent_ref,
        sems,
        result_ref,
        d_self_held,
        index_ref,
        gathered_ref,
        slope_ref,
        mean_ref,
        inverse_ref,
        pre_ref,
        d_pre_ref,
        d_mean_ref,
        total_ref,
    ) = refs[2 * domains + 9 :]
    blocks, fanout, block_rows, _ = adjacency_ref.shape
    held = [map_pool_ref, adjacency_ref, map_self_ref, w_neigh_ref, gain_ref, cotangent_ref]
    loads = [
        pltpu.make_async_copy(source, target, sems.at[i])
        for i, (source, target) in enumerate(zip(in_refs, held))
    ]
    load_index = pltpu.make_async_copy(index_in, index_ref, sems.at[len(loads) + 2])
    load_index.start()
    for load in loads[:2]:
        load.start()
    for mask in range(domains):
        for block in range(blocks):
            gathered_ref[mask * blocks + block] = piece_refs[mask][
                block * block_rows : (block + 1) * block_rows, :
            ]
    nodes, hidden = pre_ref.shape
    span = fanout * block_rows

    def wide(block):
        return jnp.concatenate([adjacency_ref[block, k] for k in range(fanout)], axis=1)

    def forward(block, _):
        sources = jnp.concatenate(
            [gathered_ref[index_ref[block * fanout + k]] for k in range(fanout)], axis=0
        )
        start = pl.multiple_of(block * span, span)
        pooled, slope_ref[pl.ds(start, span), :] = silu_parts(dot(sources, map_pool_ref[...], 1, 0))
        pooled = pooled.astype(jnp.bfloat16)
        weights = wide(block)
        inverse = 1.0 / jnp.sum(weights.astype(jnp.float32), axis=1, keepdims=True)
        own = pl.multiple_of(block * block_rows, block_rows)
        inverse_ref[pl.ds(own, block_rows), :] = jnp.broadcast_to(inverse, (block_rows, LANES))
        mean_ref[pl.ds(own, block_rows), :] = (dot(weights, pooled, 1, 0) * (0.5 * inverse)).astype(
            jnp.bfloat16
        )
        return 0

    load_index.wait()
    for load in loads[:2]:
        load.wait()
    for load in loads[2:]:
        load.start()
    lax.fori_loop(0, blocks, forward, 0)
    for load in loads[2:]:
        load.wait()
    pre_ref[...] = dot(piece_refs[0][...], map_self_ref[...], 1, 0) + dot(
        mean_ref[...], w_neigh_ref[...], 1, 0
    )
    gain = gain_ref[...].astype(jnp.float32)
    piece = 64

    def middle(part, _):
        start = pl.multiple_of(part * piece, piece)
        here = pl.ds(start, piece)
        active, slope = silu_parts(pre_ref[here, :])
        scale = lax.rsqrt(jnp.mean(active * active, axis=1, keepdims=True) + EPSILON)
        result_ref[here, :] = (active * scale * gain).astype(jnp.bfloat16)
        weighted = gain * cotangent_ref[here, :].astype(jnp.float32)
        shift = (scale * scale * scale) * jnp.mean(weighted * active, axis=1, keepdims=True)
        half_d_active = (0.5 * scale) * weighted - active * (0.5 * shift)
        d_pre_ref[here, :] = (half_d_active * slope).astype(jnp.bfloat16)
        return 0

    lax.fori_loop(0, nodes // piece, middle, 0)
    store = pltpu.make_async_copy(result_ref, node_out_ref, sems.at[len(loads)])
    store.start()
    d_pre = d_pre_ref[...]
    d_self_held[...] = 2.0 * dot(d_pre, map_self_ref[...], 1, 1)
    store_self = pltpu.make_async_copy(d_self_held, d_self_ref, sems.at[len(loads) + 1])
    store_self.start()
    d_mean_ref[...] = dot(d_pre, w_neigh_ref[...], 1, 1)
    total_ref[...] = jnp.zeros(total_ref.shape, jnp.float32)

    def backward(block, _):
        own = pl.multiple_of(block * block_rows, block_rows)
        inverse = inverse_ref[pl.ds(own, block_rows), :][:, :1]
        d_scaled = (d_mean_ref[pl.ds(own, block_rows), :] * inverse).astype(jnp.bfloat16)
        start = pl.multiple_of(block * span, span)
        share = dot(wide(block), d_scaled, 0, 0)
        d_pool = (share * slope_ref[pl.ds(start, span), :]).astype(jnp.bfloat16)
        d_source = dot(d_pool, map_pool_ref[...], 1, 1)
        for k in range(fanout):
            target = index_ref[block * fanout + k]
            total_ref[target] += d_source[k * block_rows : (k + 1) * block_rows, :]
        return 0

    lax.fori_loop(0, blocks, backward, 0)
    for mask in range(domains):
        for block in range(blocks):
            owed_refs[mask][block * block_rows : (block + 1) * block_rows, :] = total_ref[
                mask * blocks + block
            ].astype(jnp.bfloat16)
    store.wait()
    store_self.wait()


def shift(piece, mask):
    domains = lax.axis_size("dom")
    return lax.ppermute(piece, "dom", [(i, i ^ mask) for i in range(domains)])


def swap_all(buffer):
    return lax.all_to_all(buffer, ("table", "dom"), split_axis=0, concat_axis=0, tiled=True)


def body(
    tables,
    owner_ids,
    row_ids,
    neighbour_part,
    neighbour_block,
    adjacency,
    w_in,
    w_pool,
    w_self,
    w_neigh,
    out_gain,
    cotangent,
):
    groups = lax.axis_size("table")
    domains = lax.axis_size("dom")
    devices = groups * domains
    node_count, lookup_count = owner_ids.shape
    table_width = tables.shape[2]
    rows_local = tables.shape[1]
    hidden = w_self.shape[0]
    block_rows = adjacency.shape[-1]
    block_count = node_count // block_rows
    fanout = neighbour_part.shape[1]
    capacity = max(2, (2 * node_count * lookup_count + devices - 1) // devices)
    slot_count = devices * capacity
    chunks = slot_count // LANES
    f32, bf16 = jnp.float32, jnp.bfloat16

    requests, place, held = call(
        route_kernel,
        [
            on_chip((devices, capacity), jnp.int32),
            on_chip((devices, node_count), jnp.int32),
            on_chip((rows_local + SPARE, table_width), f32),
        ],
        [HBM, HBM, HBM],
        (owner_ids.T, row_ids.T, tables[0]),
        scratch=[
            pltpu.VMEM((lookup_count, node_count), jnp.int32),
            pltpu.VMEM((lookup_count, node_count), jnp.int32),
            pltpu.SemaphoreType.DMA((3,)),
        ],
    )
    flat_ids = swap_all(requests).reshape(-1)
    (fetched,) = call(
        partial(fetch_kernel, min(64, capacity)),
        [on_chip((slot_count, table_width), bf16)],
        [SMEM, CHIP],
        (flat_ids, held),
        scratch=[pltpu.VMEM((LANES, table_width), f32)],
    )
    returned = swap_all(fetched.reshape(devices, capacity, table_width))
    map_pool, map_self, cleared = call(
        prep_kernel,
        [
            in_hbm((table_width, hidden), bf16),
            in_hbm((table_width, hidden), bf16),
            on_chip((rows_local + SPARE, table_width), f32),
        ],
        [CHIP] + [HBM] * 3,
        (fetched, w_in, w_pool, w_self),
        scratch=[
            pltpu.VMEM(w_in.shape, bf16),
            pltpu.VMEM(w_pool.shape, bf16),
            pltpu.VMEM(w_self.shape, bf16),
            pltpu.SemaphoreType.DMA((3,)),
        ],
        flops=10**9,
    )
    (feature,) = call(
        combine_kernel,
        [on_chip((node_count, table_width), bf16)],
        [CHIP, CHIP, HBM],
        (place, returned.reshape(slot_count, table_width), map_pool),
    )
    half = domains // 2
    far = shift(feature, half)
    near = [shift(feature, mask) for mask in range(1, half)]
    pieces = [feature, *near, far, *[shift(far, mask) for mask in range(1, half)]]
    index = ((neighbour_part ^ lax.axis_index("dom")) * block_count + neighbour_block).reshape(-1)
    node_out, d_self, *owed = call(
        partial(sage_kernel, domains),
        [
            in_hbm((node_count, hidden), bf16, HBM),
            in_hbm((node_count, table_width), f32, HBM),
            *[on_chip((node_count, table_width), bf16) for _ in range(domains)],
        ],
        [HBM] + [CHIP] * domains + [HBM] * 6,
        (
            index,
            *pieces,
            map_pool,
            adjacency,
            map_self,
            w_neigh,
            out_gain.reshape(1, hidden),
            cotangent,
        ),
        scratch=[
            pltpu.VMEM(map_pool.shape, bf16),
            pltpu.VMEM(adjacency.shape, bf16),
            pltpu.VMEM(map_self.shape, bf16),
            pltpu.VMEM(w_neigh.shape, bf16),
            pltpu.VMEM((1, hidden), bf16),
            pltpu.VMEM(cotangent.shape, bf16),
            pltpu.SemaphoreType.DMA((9,)),
            pltpu.VMEM((node_count, hidden), bf16),
            pltpu.VMEM((node_count, table_width), f32),
            pltpu.SMEM((block_count * fanout,), jnp.int32),
            pltpu.VMEM((domains * block_count, block_rows, table_width), bf16),
            pltpu.VMEM((node_count * fanout, hidden), f32),
            pltpu.VMEM((node_count, hidden), bf16),
            pltpu.VMEM((node_count, LANES), f32),
            pltpu.VMEM((node_count, hidden), f32),
            pltpu.VMEM((node_count, hidden), bf16),
            pltpu.VMEM((node_count, hidden), f32),
            pltpu.VMEM((domains * block_count, block_rows, table_width), f32),
        ],
        flops=5 * 10**9,
    )
    relayed = [shift(owed[half + mask], mask) for mask in range(1, half)]
    back = [shift(owed[mask], mask) for mask in range(1, half)]
    relay = owed[half].astype(f32)
    for piece in relayed:
        relay = relay + piece.astype(f32)
    back = [owed[0], *back, shift(relay.astype(bf16), half)]
    (outgoing,) = call(
        spread_kernel,
        [on_chip((slot_count, table_width), bf16)],
        [CHIP, VMEM] + [CHIP] * len(back),
        (place, d_self, *back),
    )
    owed_rows = swap_all(outgoing.reshape(devices, capacity, table_width))
    _, table_grad = call(
        partial(deposit_kernel, min(16, capacity), min(64, capacity)),
        [
            on_chip((rows_local + SPARE, table_width), f32),
            in_hbm((rows_local, table_width), f32, HBM),
        ],
        [SMEM, VMEM, CHIP, CHIP],
        (
            flat_ids,
            flat_ids.reshape(chunks, LANES),
            owed_rows.reshape(slot_count, table_width),
            cleared,
        ),
        scratch=[
            pltpu.VMEM((slot_count, table_width), f32),
            pltpu.SemaphoreType.DMA,
        ],
        aliases={3: 0},
    )
    return (node_out, table_grad[None])


def solution(mesh):
    both = P(("table", "dom"), None)
    placed = (
        P("table", "dom", None),
        both,
        both,
        both,
        both,
        P(("table", "dom"), None, None, None),
        P(),
        P(),
        P(),
        P(),
        P(),
        both,
    )
    return jax.shard_map(
        body,
        mesh=mesh,
        in_specs=placed,
        out_specs=(both, P("table", "dom", None)),
        check_vma=False,
    )
```

```python
from functools import partial

import jax
import jax.numpy as jnp
from jax import lax
from jax.experimental import pallas as pl
from jax.experimental.pallas import tpu as pltpu
from jax.sharding import PartitionSpec as P

EPSILON = 1e-06
LANES = 128

VMEM = pltpu.VMEM
SMEM = pltpu.SMEM
HBM = pltpu.HBM
CHIP = "chip"
SPARE = 8


def call(kernel, outs, ins_space, args, scratch=(), flops=0, aliases=None):
    args = [
        pltpu.with_memory_space_constraint(arg, VMEM if space == CHIP else HBM)
        if space in (CHIP, HBM)
        else arg
        for space, arg in zip(ins_space, args)
    ]
    return pl.pallas_call(
        kernel,
        out_shape=[out for _, out in outs],
        in_specs=[pl.BlockSpec(memory_space=VMEM if s == CHIP else s) for s in ins_space],
        out_specs=[pl.BlockSpec(memory_space=space) for space, _ in outs],
        scratch_shapes=list(scratch),
        input_output_aliases=aliases or {},
        compiler_params=pltpu.CompilerParams(vmem_limit_bytes=40 << 20),
        cost_estimate=pl.CostEstimate(flops=flops, transcendentals=0, bytes_accessed=1 << 20),
    )(*args)


def on_chip(shape, dtype):
    return VMEM, pltpu.VMEM(shape, dtype)


def in_hbm(shape, dtype, space=VMEM):
    return space, jax.ShapeDtypeStruct(shape, dtype)


def dot(left, right, left_dim, right_dim):
    return lax.dot_general(
        left, right, (((left_dim,), (right_dim,)), ((), ())), preferred_element_type=jnp.float32
    )


def ones_where(mask):
    return jnp.where(mask, 1.0, 0.0).astype(jnp.bfloat16)


def silu_parts(half):
    upper = jnp.tanh(half) + 1.0
    value = half * upper
    return value, upper + value * (2.0 - upper)


def route_kernel(
    owner_in, row_in, table_ref, request_ref, place_ref, held_ref, owner_ref, row_ref, sems
):
    owner_load = pltpu.make_async_copy(owner_in, owner_ref, sems.at[0])
    row_load = pltpu.make_async_copy(row_in, row_ref, sems.at[1])
    load = pltpu.make_async_copy(
        table_ref, held_ref.at[pl.ds(SPARE, table_ref.shape[0]), :], sems.at[2]
    )
    owner_load.start()
    row_load.start()
    load.start()
    held_ref[:SPARE, :] = jnp.zeros((SPARE, held_ref.shape[1]), jnp.float32)
    lookups, nodes = owner_ref.shape
    devices, capacity = request_ref.shape
    owners = lax.broadcasted_iota(jnp.int32, (devices, nodes), 0)
    earlier = ones_where(
        lax.broadcasted_iota(jnp.int32, (nodes, nodes), 0)
        < lax.broadcasted_iota(jnp.int32, (nodes, nodes), 1)
    )
    owner_load.wait()
    row_load.wait()
    hits = [owner_ref[j : j + 1, :] == owners for j in range(lookups)]
    before = dot(jnp.concatenate([ones_where(hit) for hit in hits], axis=0), earlier, 1, 0)
    carry = jnp.zeros((devices, 1), jnp.float32)
    place = jnp.zeros((devices, nodes), jnp.float32)
    slots = lax.broadcasted_iota(jnp.int32, (capacity, nodes), 0).astype(jnp.float32)
    high, low, taken = [], [], []
    for j in range(lookups):
        position = before[j * devices : (j + 1) * devices, :] + carry
        carry = carry + jnp.sum(jnp.where(hits[j], 1.0, 0.0), axis=1, keepdims=True)
        place = place + jnp.where(hits[j], position + 1.0, 0.0)
        own = jnp.sum(jnp.where(hits[j], position, 0.0), axis=0, keepdims=True)
        taken.append(ones_where(own == slots))
        row = row_ref[j : j + 1, :] + 1
        upper = (row >> 7).astype(jnp.float32)
        lower = (row & 127).astype(jnp.float32)
        high.append(jnp.where(hits[j], upper, 0.0).astype(jnp.bfloat16))
        low.append(jnp.where(hits[j], lower, 0.0).astype(jnp.bfloat16))
    taken = jnp.concatenate(taken, axis=1)
    request = dot(jnp.concatenate(high, axis=1), taken, 1, 1) * 128.0 + dot(
        jnp.concatenate(low, axis=1), taken, 1, 1
    )
    request_ref[...] = request.astype(jnp.int32)
    place_ref[...] = place.astype(jnp.int32) - 1
    load.wait()


def prep_kernel(
    _,
    w_in_ref,
    w_pool_ref,
    w_self_ref,
    map_pool_ref,
    map_self_ref,
    sums_ref,
    w_in_held,
    w_pool_held,
    w_self_held,
    sems,
):
    copies = [
        pltpu.make_async_copy(source, target, sems.at[i])
        for i, (source, target) in enumerate(
            [(w_in_ref, w_in_held), (w_pool_ref, w_pool_held), (w_self_ref, w_self_held)]
        )
    ]
    for copy in copies:
        copy.start()

    def clear(i, _):
        start = pl.multiple_of(i * 64, 64)
        sums_ref[pl.ds(start, 64), :] = jnp.zeros((64, sums_ref.shape[1]), jnp.float32)
        return 0

    whole = sums_ref.shape[0] // 64
    lax.fori_loop(0, whole, clear, 0)
    rest = sums_ref.shape[0] - whole * 64
    if rest:
        sums_ref[whole * 64 :, :] = jnp.zeros((rest, sums_ref.shape[1]), jnp.float32)
    copies[0].wait()
    copies[1].wait()
    map_pool_ref[...] = (0.5 * dot(w_in_held[...], w_pool_held[...], 1, 0)).astype(jnp.bfloat16)
    copies[2].wait()
    map_self_ref[...] = (0.5 * dot(w_in_held[...], w_self_held[...], 1, 0)).astype(jnp.bfloat16)


def fetch_kernel(size, id_ref, table_ref, out_ref, rows_ref):
    chunks = out_ref.shape[0] // LANES
    rows_ref[...] = jnp.zeros(rows_ref.shape, jnp.float32)

    def step(chunk, _):
        for group in range(LANES // size):
            base = chunk * LANES + group * size

            @pl.when(id_ref[base] > 0)
            def _():
                for i in range(size):
                    row = id_ref[base + i] + (SPARE - 1)
                    rows_ref[pl.ds(group * size + i, 1), :] = table_ref[pl.ds(row, 1), :]

        start = pl.multiple_of(chunk * LANES, LANES)
        out_ref[pl.ds(start, LANES), :] = rows_ref[...].astype(jnp.bfloat16)
        return 0

    lax.fori_loop(0, chunks, step, 0)


def select_rows(place_ref, first, count, capacity):
    nodes = place_ref.shape[1]
    slots = lax.broadcasted_iota(jnp.int32, (capacity, nodes), 0)
    parts = [ones_where(place_ref[o : o + 1, :] == slots) for o in range(first, first + count)]
    return jnp.concatenate(parts, axis=0)


def combine_kernel(place_ref, returned_ref, _, feature_ref):
    devices = place_ref.shape[0]
    capacity = returned_ref.shape[0] // devices
    count = max(1, 512 // capacity)
    total = None
    for first in range(0, devices, count):
        chosen = select_rows(place_ref, first, count, capacity)
        rows = returned_ref[first * capacity : (first + count) * capacity, :]
        part = dot(rows, chosen, 0, 0)
        total = part if total is None else total + part
    feature_ref[...] = total.T.astype(jnp.bfloat16)


def spread_kernel(place_ref, d_self_ref, *refs):
    *back_refs, out_ref = refs
    devices = place_ref.shape[0]
    capacity = out_ref.shape[0] // devices
    count = max(1, 512 // capacity)
    total = d_self_ref[...]
    for back_ref in back_refs:
        total = total + back_ref[...].astype(jnp.float32)
    d_feature = total.astype(jnp.bfloat16)
    for first in range(0, devices, count):
        chosen = select_rows(place_ref, first, count, capacity)
        out_ref[first * capacity : (first + count) * capacity, :] = dot(
            chosen, d_feature, 1, 0
        ).astype(jnp.bfloat16)


def deposit_kernel(
    size, gate, flat_in, ids_in, grad_ref, _, sums_ref, out_ref, fresh_ref, id_ref, ids_ref, sems
):
    chunks = ids_ref.shape[0]
    load_ids = pltpu.make_async_copy(ids_in, ids_ref, sems.at[1])
    load = pltpu.make_async_copy(flat_in, id_ref, sems.at[2])
    load_ids.start()
    load.start()
    load_ids.wait()
    rows = ids_ref[...].astype(jnp.float32)
    columns = rows.T
    same_group = (
        lax.broadcasted_iota(jnp.int32, (LANES, LANES), 0) // size
        == lax.broadcasted_iota(jnp.int32, (LANES, LANES), 1) // size
    )
    for chunk in range(chunks):
        same = (columns[:, chunk : chunk + 1] == rows[chunk : chunk + 1, :]) & same_group
        fresh_ref[chunk * LANES : (chunk + 1) * LANES, :] = dot(
            ones_where(same), grad_ref[chunk * LANES : (chunk + 1) * LANES, :], 1, 0
        )

    def step(chunk, _):
        for part in range(LANES // gate):
            first = chunk * LANES + part * gate

            @pl.when(id_ref[first] > 0)
            def _():
                for group in range(gate // size):
                    base = first + group * size
                    targets = [id_ref[base + i] + (SPARE - 1) for i in range(size)]
                    fresh = [
                        sums_ref[pl.ds(targets[i], 1), :] + fresh_ref[pl.ds(base + i, 1), :]
                        for i in range(size)
                    ]
                    for i in range(size):
                        sums_ref[pl.ds(targets[i], 1), :] = fresh[i]

        return 0

    load.wait()
    lax.fori_loop(0, chunks, step, 0)
    store = pltpu.make_async_copy(sums_ref.at[pl.ds(SPARE, out_ref.shape[0]), :], out_ref, sems.at[0])
    store.start()
    store.wait()


def sage_kernel(domains, *refs):
    index_in, *piece_refs = refs[: domains + 1]
    in_refs = refs[domains + 1 : domains + 7]
    node_out_ref, d_self_ref, *owed_refs = refs[domains + 7 : 2 * domains + 9]
    (
        map_pool_ref,
        adjacency_ref,
        map_self_ref,
        w_neigh_ref,
        gain_ref,
        cotangent_ref,
        sems,
        result_ref,
        d_self_held,
        index_ref,
        gathered_ref,
        slope_ref,
        mean_ref,
        inverse_ref,
        pre_ref,
        d_pre_ref,
        d_mean_ref,
        total_ref,
    ) = refs[2 * domains + 9 :]
    blocks, fanout, block_rows, _ = adjacency_ref.shape
    held = [map_pool_ref, adjacency_ref, map_self_ref, w_neigh_ref, gain_ref, cotangent_ref]
    loads = [
        pltpu.make_async_copy(source, target, sems.at[i])
        for i, (source, target) in enumerate(zip(in_refs, held))
    ]
    load_index = pltpu.make_async_copy(index_in, index_ref, sems.at[len(loads) + 2])
    load_index.start()
    for load in loads[:2]:
        load.start()
    for mask in range(domains):
        for block in range(blocks):
            gathered_ref[mask * blocks + block] = piece_refs[mask][
                block * block_rows : (block + 1) * block_rows, :
            ]
    nodes, hidden = pre_ref.shape
    span = fanout * block_rows

    def wide(block):
        return jnp.concatenate([adjacency_ref[block, k] for k in range(fanout)], axis=1)

    def forward(block, _):
        sources = jnp.concatenate(
            [gathered_ref[index_ref[block * fanout + k]] for k in range(fanout)], axis=0
        )
        start = pl.multiple_of(block * span, span)
        pooled, slope_ref[pl.ds(start, span), :] = silu_parts(dot(sources, map_pool_ref[...], 1, 0))
        pooled = pooled.astype(jnp.bfloat16)
        weights = wide(block)
        inverse = 1.0 / jnp.sum(weights.astype(jnp.float32), axis=1, keepdims=True)
        own = pl.multiple_of(block * block_rows, block_rows)
        inverse_ref[pl.ds(own, block_rows), :] = jnp.broadcast_to(inverse, (block_rows, LANES))
        mean_ref[pl.ds(own, block_rows), :] = (dot(weights, pooled, 1, 0) * (0.5 * inverse)).astype(
            jnp.bfloat16
        )
        return 0

    load_index.wait()
    for load in loads[:2]:
        load.wait()
    for load in loads[2:]:
        load.start()
    lax.fori_loop(0, blocks, forward, 0, unroll=2)
    for load in loads[2:]:
        load.wait()
    pre_ref[...] = dot(piece_refs[0][...], map_self_ref[...], 1, 0) + dot(
        mean_ref[...], w_neigh_ref[...], 1, 0
    )
    gain = gain_ref[...].astype(jnp.float32)
    piece = 128

    def middle(part, _):
        start = pl.multiple_of(part * piece, piece)
        here = pl.ds(start, piece)
        active, slope = silu_parts(pre_ref[here, :])
        scale = lax.rsqrt(jnp.mean(active * active, axis=1, keepdims=True) + EPSILON)
        result_ref[here, :] = (active * scale * gain).astype(jnp.bfloat16)
        weighted = gain * cotangent_ref[here, :].astype(jnp.float32)
        shift = (scale * scale * scale) * jnp.mean(weighted * active, axis=1, keepdims=True)
        half_d_active = (0.5 * scale) * weighted - active * (0.5 * shift)
        d_pre_ref[here, :] = (half_d_active * slope).astype(jnp.bfloat16)
        return 0

    lax.fori_loop(0, nodes // piece, middle, 0)
    store = pltpu.make_async_copy(result_ref, node_out_ref, sems.at[len(loads)])
    store.start()
    d_pre = d_pre_ref[...]
    d_self_held[...] = 2.0 * dot(d_pre, map_self_ref[...], 1, 1)
    store_self = pltpu.make_async_copy(d_self_held, d_self_ref, sems.at[len(loads) + 1])
    store_self.start()
    d_mean_ref[...] = dot(d_pre, w_neigh_ref[...], 1, 1)
    total_ref[...] = jnp.zeros(total_ref.shape, jnp.float32)

    def backward(block, _):
        own = pl.multiple_of(block * block_rows, block_rows)
        inverse = inverse_ref[pl.ds(own, block_rows), :][:, :1]
        d_scaled = (d_mean_ref[pl.ds(own, block_rows), :] * inverse).astype(jnp.bfloat16)
        start = pl.multiple_of(block * span, span)
        share = dot(wide(block), d_scaled, 0, 0)
        d_pool = (share * slope_ref[pl.ds(start, span), :]).astype(jnp.bfloat16)
        d_source = dot(d_pool, map_pool_ref[...], 1, 1)
        for k in range(fanout):
            target = index_ref[block * fanout + k]
            total_ref[target] += d_source[k * block_rows : (k + 1) * block_rows, :]
        return 0

    lax.fori_loop(0, blocks, backward, 0, unroll=2)
    for mask in range(domains):
        for block in range(blocks):
            owed_refs[mask][block * block_rows : (block + 1) * block_rows, :] = total_ref[
                mask * blocks + block
            ].astype(jnp.bfloat16)
    store.wait()
    store_self.wait()


def shift(piece, mask):
    domains = lax.axis_size("dom")
    return lax.ppermute(piece, "dom", [(i, i ^ mask) for i in range(domains)])


def swap_all(buffer):
    return lax.all_to_all(buffer, ("table", "dom"), split_axis=0, concat_axis=0, tiled=True)


def body(
    tables,
    owner_ids,
    row_ids,
    neighbour_part,
    neighbour_block,
    adjacency,
    w_in,
    w_pool,
    w_self,
    w_neigh,
    out_gain,
    cotangent,
):
    groups = lax.axis_size("table")
    domains = lax.axis_size("dom")
    devices = groups * domains
    node_count, lookup_count = owner_ids.shape
    table_width = tables.shape[2]
    rows_local = tables.shape[1]
    hidden = w_self.shape[0]
    block_rows = adjacency.shape[-1]
    block_count = node_count // block_rows
    fanout = neighbour_part.shape[1]
    capacity = max(2, (2 * node_count * lookup_count + devices - 1) // devices)
    slot_count = devices * capacity
    chunks = slot_count // LANES
    f32, bf16 = jnp.float32, jnp.bfloat16

    requests, place, held = call(
        route_kernel,
        [
            on_chip((devices, capacity), jnp.int32),
            on_chip((devices, node_count), jnp.int32),
            on_chip((rows_local + SPARE, table_width), f32),
        ],
        [HBM, HBM, HBM],
        (owner_ids.T, row_ids.T, tables[0]),
        scratch=[
            pltpu.VMEM((lookup_count, node_count), jnp.int32),
            pltpu.VMEM((lookup_count, node_count), jnp.int32),
            pltpu.SemaphoreType.DMA((3,)),
        ],
    )
    flat_ids = swap_all(requests).reshape(-1)
    (fetched,) = call(
        partial(fetch_kernel, min(64, capacity)),
        [on_chip((slot_count, table_width), bf16)],
        [SMEM, CHIP],
        (flat_ids, held),
        scratch=[pltpu.VMEM((LANES, table_width), f32)],
    )
    returned = swap_all(fetched.reshape(devices, capacity, table_width))
    map_pool, map_self, cleared = call(
        prep_kernel,
        [
            in_hbm((table_width, hidden), bf16),
            in_hbm((table_width, hidden), bf16),
            on_chip((rows_local + SPARE, table_width), f32),
        ],
        [CHIP] + [HBM] * 3,
        (fetched, w_in, w_pool, w_self),
        scratch=[
            pltpu.VMEM(w_in.shape, bf16),
            pltpu.VMEM(w_pool.shape, bf16),
            pltpu.VMEM(w_self.shape, bf16),
            pltpu.SemaphoreType.DMA((3,)),
        ],
        flops=10**9,
    )
    (feature,) = call(
        combine_kernel,
        [on_chip((node_count, table_width), bf16)],
        [CHIP, CHIP, HBM],
        (place, returned.reshape(slot_count, table_width), map_pool),
    )
    half = domains // 2
    far = shift(feature, half)
    near = [shift(feature, mask) for mask in range(1, half)]
    pieces = [feature, *near, far, *[shift(far, mask) for mask in range(1, half)]]
    index = ((neighbour_part ^ lax.axis_index("dom")) * block_count + neighbour_block).reshape(-1)
    node_out, d_self, *owed = call(
        partial(sage_kernel, domains),
        [
            in_hbm((node_count, hidden), bf16, HBM),
            in_hbm((node_count, table_width), f32, HBM),
            *[on_chip((node_count, table_width), bf16) for _ in range(domains)],
        ],
        [HBM] + [CHIP] * domains + [HBM] * 6,
        (
            index,
            *pieces,
            map_pool,
            adjacency,
            map_self,
            w_neigh,
            out_gain.reshape(1, hidden),
            cotangent,
        ),
        scratch=[
            pltpu.VMEM(map_pool.shape, bf16),
            pltpu.VMEM(adjacency.shape, bf16),
            pltpu.VMEM(map_self.shape, bf16),
            pltpu.VMEM(w_neigh.shape, bf16),
            pltpu.VMEM((1, hidden), bf16),
            pltpu.VMEM(cotangent.shape, bf16),
            pltpu.SemaphoreType.DMA((9,)),
            pltpu.VMEM((node_count, hidden), bf16),
            pltpu.VMEM((node_count, table_width), f32),
            pltpu.SMEM((block_count * fanout,), jnp.int32),
            pltpu.VMEM((domains * block_count, block_rows, table_width), bf16),
            pltpu.VMEM((node_count * fanout, hidden), f32),
            pltpu.VMEM((node_count, hidden), bf16),
            pltpu.VMEM((node_count, LANES), f32),
            pltpu.VMEM((node_count, hidden), f32),
            pltpu.VMEM((node_count, hidden), bf16),
            pltpu.VMEM((node_count, hidden), f32),
            pltpu.VMEM((domains * block_count, block_rows, table_width), f32),
        ],
        flops=5 * 10**9,
    )
    relayed = [shift(owed[half + mask], mask) for mask in range(1, half)]
    back = [shift(owed[mask], mask) for mask in range(1, half)]
    relay = owed[half].astype(f32)
    for piece in relayed:
        relay = relay + piece.astype(f32)
    back = [owed[0], *back, shift(relay.astype(bf16), half)]
    (outgoing,) = call(
        spread_kernel,
        [on_chip((slot_count, table_width), bf16)],
        [CHIP, VMEM] + [CHIP] * len(back),
        (place, d_self, *back),
    )
    owed_rows = swap_all(outgoing.reshape(devices, capacity, table_width))
    _, table_grad = call(
        partial(deposit_kernel, min(16, capacity), min(64, capacity)),
        [
            on_chip((rows_local + SPARE, table_width), f32),
            in_hbm((rows_local, table_width), f32, HBM),
        ],
        [HBM, HBM, CHIP, CHIP],
        (
            flat_ids,
            flat_ids.reshape(chunks, LANES),
            owed_rows.reshape(slot_count, table_width),
            cleared,
        ),
        scratch=[
            pltpu.VMEM((slot_count, table_width), f32),
            pltpu.SMEM((slot_count,), jnp.int32),
            pltpu.VMEM((chunks, LANES), jnp.int32),
            pltpu.SemaphoreType.DMA((3,)),
        ],
        aliases={3: 0},
    )
    return (node_out, table_grad[None])


def solution(mesh):
    both = P(("table", "dom"), None)
    placed = (
        P("table", "dom", None),
        both,
        both,
        both,
        both,
        P(("table", "dom"), None, None, None),
        P(),
        P(),
        P(),
        P(),
        P(),
        both,
    )
    return jax.shard_map(
        body,
        mesh=mesh,
        in_specs=placed,
        out_specs=(both, P("table", "dom", None)),
        check_vma=False,
    )
```

```python
from functools import partial

import jax
import jax.numpy as jnp
from jax import lax
from jax.experimental import pallas as pl
from jax.experimental.pallas import tpu as pltpu
from jax.sharding import PartitionSpec as P

EPSILON = 1e-06
LANES = 128

VMEM = pltpu.VMEM
SMEM = pltpu.SMEM
HBM = pltpu.HBM
CHIP = "chip"
SPARE = 8


def call(kernel, outs, ins_space, args, scratch=(), flops=0, aliases=None):
    args = [
        pltpu.with_memory_space_constraint(arg, VMEM if space == CHIP else HBM)
        if space in (CHIP, HBM)
        else arg
        for space, arg in zip(ins_space, args)
    ]
    return pl.pallas_call(
        kernel,
        out_shape=[out for _, out in outs],
        in_specs=[pl.BlockSpec(memory_space=VMEM if s == CHIP else s) for s in ins_space],
        out_specs=[pl.BlockSpec(memory_space=space) for space, _ in outs],
        scratch_shapes=list(scratch),
        input_output_aliases=aliases or {},
        compiler_params=pltpu.CompilerParams(vmem_limit_bytes=40 << 20),
        cost_estimate=pl.CostEstimate(flops=flops, transcendentals=0, bytes_accessed=1 << 20),
    )(*args)


def on_chip(shape, dtype):
    return VMEM, pltpu.VMEM(shape, dtype)


def in_hbm(shape, dtype, space=VMEM):
    return space, jax.ShapeDtypeStruct(shape, dtype)


def dot(left, right, left_dim, right_dim):
    return lax.dot_general(
        left, right, (((left_dim,), (right_dim,)), ((), ())), preferred_element_type=jnp.float32
    )


def ones_where(mask):
    return jnp.where(mask, 1.0, 0.0).astype(jnp.bfloat16)


def silu_parts(half):
    upper = jnp.tanh(half) + 1.0
    value = half * upper
    return value, upper + value * (2.0 - upper)


def route_kernel(
    owner_in, row_in, table_ref, request_ref, place_ref, held_ref, owner_ref, row_ref, sems
):
    owner_load = pltpu.make_async_copy(owner_in, owner_ref, sems.at[0])
    row_load = pltpu.make_async_copy(row_in, row_ref, sems.at[1])
    load = pltpu.make_async_copy(
        table_ref, held_ref.at[pl.ds(SPARE, table_ref.shape[0]), :], sems.at[2]
    )
    owner_load.start()
    row_load.start()
    load.start()
    held_ref[:SPARE, :] = jnp.zeros((SPARE, held_ref.shape[1]), jnp.float32)
    lookups, nodes = owner_ref.shape
    devices, capacity = request_ref.shape
    owners = lax.broadcasted_iota(jnp.int32, (devices, nodes), 0)
    earlier = ones_where(
        lax.broadcasted_iota(jnp.int32, (nodes, nodes), 0)
        < lax.broadcasted_iota(jnp.int32, (nodes, nodes), 1)
    )
    owner_load.wait()
    row_load.wait()
    hits = [owner_ref[j : j + 1, :] == owners for j in range(lookups)]
    before = dot(jnp.concatenate([ones_where(hit) for hit in hits], axis=0), earlier, 1, 0)
    carry = jnp.zeros((devices, 1), jnp.float32)
    place = jnp.zeros((devices, nodes), jnp.float32)
    slots = lax.broadcasted_iota(jnp.int32, (capacity, nodes), 0).astype(jnp.float32)
    high, low, taken = [], [], []
    for j in range(lookups):
        position = before[j * devices : (j + 1) * devices, :] + carry
        carry = carry + jnp.sum(jnp.where(hits[j], 1.0, 0.0), axis=1, keepdims=True)
        place = place + jnp.where(hits[j], position + 1.0, 0.0)
        own = jnp.sum(jnp.where(hits[j], position, 0.0), axis=0, keepdims=True)
        taken.append(ones_where(own == slots))
        row = row_ref[j : j + 1, :] + 1
        upper = (row >> 7).astype(jnp.float32)
        lower = (row & 127).astype(jnp.float32)
        high.append(jnp.where(hits[j], upper, 0.0).astype(jnp.bfloat16))
        low.append(jnp.where(hits[j], lower, 0.0).astype(jnp.bfloat16))
    taken = jnp.concatenate(taken, axis=1)
    request = dot(jnp.concatenate(high, axis=1), taken, 1, 1) * 128.0 + dot(
        jnp.concatenate(low, axis=1), taken, 1, 1
    )
    request_ref[...] = request.astype(jnp.int32)
    place_ref[...] = place.astype(jnp.int32) - 1
    load.wait()


def prep_kernel(
    _,
    w_in_ref,
    w_pool_ref,
    w_self_ref,
    map_pool_ref,
    map_self_ref,
    sums_ref,
    w_in_held,
    w_pool_held,
    w_self_held,
    sems,
):
    copies = [
        pltpu.make_async_copy(source, target, sems.at[i])
        for i, (source, target) in enumerate(
            [(w_in_ref, w_in_held), (w_pool_ref, w_pool_held), (w_self_ref, w_self_held)]
        )
    ]
    for copy in copies:
        copy.start()

    def clear(i, _):
        start = pl.multiple_of(i * 64, 64)
        sums_ref[pl.ds(start, 64), :] = jnp.zeros((64, sums_ref.shape[1]), jnp.float32)
        return 0

    whole = sums_ref.shape[0] // 64
    lax.fori_loop(0, whole, clear, 0)
    rest = sums_ref.shape[0] - whole * 64
    if rest:
        sums_ref[whole * 64 :, :] = jnp.zeros((rest, sums_ref.shape[1]), jnp.float32)
    copies[0].wait()
    copies[1].wait()
    map_pool_ref[...] = (0.5 * dot(w_in_held[...], w_pool_held[...], 1, 0)).astype(jnp.bfloat16)
    copies[2].wait()
    map_self_ref[...] = (0.5 * dot(w_in_held[...], w_self_held[...], 1, 0)).astype(jnp.bfloat16)


def warm_kernel(_, pool_in, adjacency_in, pool_out, adjacency_out, sems):
    loads = [
        pltpu.make_async_copy(pool_in, pool_out, sems.at[0]),
        pltpu.make_async_copy(adjacency_in, adjacency_out, sems.at[1]),
    ]
    for load in loads:
        load.start()
    for load in loads:
        load.wait()


def fetch_kernel(size, id_ref, table_ref, out_ref, rows_ref):
    chunks = out_ref.shape[0] // LANES
    rows_ref[...] = jnp.zeros(rows_ref.shape, jnp.float32)

    def step(chunk, _):
        for group in range(LANES // size):
            base = chunk * LANES + group * size

            @pl.when(id_ref[base] > 0)
            def _():
                for i in range(size):
                    row = id_ref[base + i] + (SPARE - 1)
                    rows_ref[pl.ds(group * size + i, 1), :] = table_ref[pl.ds(row, 1), :]

        start = pl.multiple_of(chunk * LANES, LANES)
        out_ref[pl.ds(start, LANES), :] = rows_ref[...].astype(jnp.bfloat16)
        return 0

    lax.fori_loop(0, chunks, step, 0)


def select_rows(place_ref, first, count, capacity):
    nodes = place_ref.shape[1]
    slots = lax.broadcasted_iota(jnp.int32, (capacity, nodes), 0)
    parts = [ones_where(place_ref[o : o + 1, :] == slots) for o in range(first, first + count)]
    return jnp.concatenate(parts, axis=0)


def combine_kernel(place_ref, returned_ref, _, feature_ref):
    devices = place_ref.shape[0]
    capacity = returned_ref.shape[0] // devices
    count = max(1, 512 // capacity)
    total = None
    for first in range(0, devices, count):
        chosen = select_rows(place_ref, first, count, capacity)
        rows = returned_ref[first * capacity : (first + count) * capacity, :]
        part = dot(rows, chosen, 0, 0)
        total = part if total is None else total + part
    feature_ref[...] = total.T.astype(jnp.bfloat16)


def spread_kernel(place_ref, d_self_ref, *refs):
    *back_refs, out_ref = refs
    devices = place_ref.shape[0]
    capacity = out_ref.shape[0] // devices
    count = max(1, 512 // capacity)
    total = d_self_ref[...]
    for back_ref in back_refs:
        total = total + back_ref[...].astype(jnp.float32)
    d_feature = total.astype(jnp.bfloat16)
    for first in range(0, devices, count):
        chosen = select_rows(place_ref, first, count, capacity)
        out_ref[first * capacity : (first + count) * capacity, :] = dot(
            chosen, d_feature, 1, 0
        ).astype(jnp.bfloat16)


def deposit_kernel(
    size, gate, flat_in, ids_in, grad_ref, _, sums_ref, out_ref, fresh_ref, id_ref, ids_ref, sems
):
    chunks = ids_ref.shape[0]
    load_ids = pltpu.make_async_copy(ids_in, ids_ref, sems.at[1])
    load = pltpu.make_async_copy(flat_in, id_ref, sems.at[2])
    load_ids.start()
    load.start()
    load_ids.wait()
    rows = ids_ref[...].astype(jnp.float32)
    columns = rows.T
    same_group = (
        lax.broadcasted_iota(jnp.int32, (LANES, LANES), 0) // size
        == lax.broadcasted_iota(jnp.int32, (LANES, LANES), 1) // size
    )
    for chunk in range(chunks):
        same = (columns[:, chunk : chunk + 1] == rows[chunk : chunk + 1, :]) & same_group
        fresh_ref[chunk * LANES : (chunk + 1) * LANES, :] = dot(
            ones_where(same), grad_ref[chunk * LANES : (chunk + 1) * LANES, :], 1, 0
        )

    def step(chunk, _):
        for part in range(LANES // gate):
            first = chunk * LANES + part * gate

            @pl.when(id_ref[first] > 0)
            def _():
                for group in range(gate // size):
                    base = first + group * size
                    targets = [id_ref[base + i] + (SPARE - 1) for i in range(size)]
                    fresh = [
                        sums_ref[pl.ds(targets[i], 1), :] + fresh_ref[pl.ds(base + i, 1), :]
                        for i in range(size)
                    ]
                    for i in range(size):
                        sums_ref[pl.ds(targets[i], 1), :] = fresh[i]

        return 0

    load.wait()
    lax.fori_loop(0, chunks, step, 0)
    store = pltpu.make_async_copy(sums_ref.at[pl.ds(SPARE, out_ref.shape[0]), :], out_ref, sems.at[0])
    store.start()
    store.wait()


def sage_kernel(domains, *refs):
    index_in, *piece_refs = refs[: domains + 1]
    map_pool_ref, adjacency_ref, *in_refs = refs[domains + 1 : domains + 7]
    node_out_ref, d_self_ref, *owed_refs = refs[domains + 7 : 2 * domains + 9]
    (
        map_self_ref,
        w_neigh_ref,
        gain_ref,
        cotangent_ref,
        sems,
        result_ref,
        d_self_held,
        index_ref,
        gathered_ref,
        slope_ref,
        mean_ref,
        inverse_ref,
        pre_ref,
        d_pre_ref,
        d_mean_ref,
        total_ref,
    ) = refs[2 * domains + 9 :]
    blocks, fanout, block_rows, _ = adjacency_ref.shape
    held = [map_self_ref, w_neigh_ref, gain_ref, cotangent_ref]
    loads = [
        pltpu.make_async_copy(source, target, sems.at[i])
        for i, (source, target) in enumerate(zip(in_refs, held))
    ]
    load_index = pltpu.make_async_copy(index_in, index_ref, sems.at[len(loads) + 2])
    load_index.start()
    for load in loads:
        load.start()
    for mask in range(domains):
        for block in range(blocks):
            gathered_ref[mask * blocks + block] = piece_refs[mask][
                block * block_rows : (block + 1) * block_rows, :
            ]
    nodes, hidden = pre_ref.shape
    span = fanout * block_rows

    def wide(block):
        return jnp.concatenate([adjacency_ref[block, k] for k in range(fanout)], axis=1)

    def forward(block, _):
        sources = jnp.concatenate(
            [gathered_ref[index_ref[block * fanout + k]] for k in range(fanout)], axis=0
        )
        start = pl.multiple_of(block * span, span)
        pooled, slope_ref[pl.ds(start, span), :] = silu_parts(dot(sources, map_pool_ref[...], 1, 0))
        pooled = pooled.astype(jnp.bfloat16)
        weights = wide(block)
        inverse = 1.0 / jnp.sum(weights.astype(jnp.float32), axis=1, keepdims=True)
        own = pl.multiple_of(block * block_rows, block_rows)
        inverse_ref[pl.ds(own, block_rows), :] = jnp.broadcast_to(inverse, (block_rows, LANES))
        mean_ref[pl.ds(own, block_rows), :] = (dot(weights, pooled, 1, 0) * (0.5 * inverse)).astype(
            jnp.bfloat16
        )
        return 0

    load_index.wait()
    lax.fori_loop(0, blocks, forward, 0, unroll=2)
    for load in loads:
        load.wait()
    pre_ref[...] = dot(piece_refs[0][...], map_self_ref[...], 1, 0) + dot(
        mean_ref[...], w_neigh_ref[...], 1, 0
    )
    gain = gain_ref[...].astype(jnp.float32)
    piece = 128

    def middle(part, _):
        start = pl.multiple_of(part * piece, piece)
        here = pl.ds(start, piece)
        active, slope = silu_parts(pre_ref[here, :])
        scale = lax.rsqrt(jnp.mean(active * active, axis=1, keepdims=True) + EPSILON)
        result_ref[here, :] = (active * scale * gain).astype(jnp.bfloat16)
        weighted = gain * cotangent_ref[here, :].astype(jnp.float32)
        shift = (scale * scale * scale) * jnp.mean(weighted * active, axis=1, keepdims=True)
        half_d_active = (0.5 * scale) * weighted - active * (0.5 * shift)
        d_pre_ref[here, :] = (half_d_active * slope).astype(jnp.bfloat16)
        return 0

    lax.fori_loop(0, nodes // piece, middle, 0)
    store = pltpu.make_async_copy(result_ref, node_out_ref, sems.at[len(loads)])
    store.start()
    d_pre = d_pre_ref[...]
    d_self_held[...] = 2.0 * dot(d_pre, map_self_ref[...], 1, 1)
    store_self = pltpu.make_async_copy(d_self_held, d_self_ref, sems.at[len(loads) + 1])
    store_self.start()
    d_mean_ref[...] = dot(d_pre, w_neigh_ref[...], 1, 1)
    total_ref[...] = jnp.zeros(total_ref.shape, jnp.float32)

    def backward(block, _):
        own = pl.multiple_of(block * block_rows, block_rows)
        inverse = inverse_ref[pl.ds(own, block_rows), :][:, :1]
        d_scaled = (d_mean_ref[pl.ds(own, block_rows), :] * inverse).astype(jnp.bfloat16)
        start = pl.multiple_of(block * span, span)
        share = dot(wide(block), d_scaled, 0, 0)
        d_pool = (share * slope_ref[pl.ds(start, span), :]).astype(jnp.bfloat16)
        d_source = dot(d_pool, map_pool_ref[...], 1, 1)
        for k in range(fanout):
            target = index_ref[block * fanout + k]
            total_ref[target] += d_source[k * block_rows : (k + 1) * block_rows, :]
        return 0

    lax.fori_loop(0, blocks, backward, 0, unroll=2)
    for mask in range(domains):
        for block in range(blocks):
            owed_refs[mask][block * block_rows : (block + 1) * block_rows, :] = total_ref[
                mask * blocks + block
            ].astype(jnp.bfloat16)
    store.wait()
    store_self.wait()


def shift(piece, mask):
    domains = lax.axis_size("dom")
    return lax.ppermute(piece, "dom", [(i, i ^ mask) for i in range(domains)])


def swap_all(buffer):
    return lax.all_to_all(buffer, ("table", "dom"), split_axis=0, concat_axis=0, tiled=True)


def body(
    tables,
    owner_ids,
    row_ids,
    neighbour_part,
    neighbour_block,
    adjacency,
    w_in,
    w_pool,
    w_self,
    w_neigh,
    out_gain,
    cotangent,
):
    groups = lax.axis_size("table")
    domains = lax.axis_size("dom")
    devices = groups * domains
    node_count, lookup_count = owner_ids.shape
    table_width = tables.shape[2]
    rows_local = tables.shape[1]
    hidden = w_self.shape[0]
    block_rows = adjacency.shape[-1]
    block_count = node_count // block_rows
    fanout = neighbour_part.shape[1]
    capacity = max(2, (2 * node_count * lookup_count + devices - 1) // devices)
    slot_count = devices * capacity
    chunks = slot_count // LANES
    f32, bf16 = jnp.float32, jnp.bfloat16

    requests, place, held = call(
        route_kernel,
        [
            on_chip((devices, capacity), jnp.int32),
            on_chip((devices, node_count), jnp.int32),
            on_chip((rows_local + SPARE, table_width), f32),
        ],
        [HBM, HBM, HBM],
        (owner_ids.T, row_ids.T, tables[0]),
        scratch=[
            pltpu.VMEM((lookup_count, node_count), jnp.int32),
            pltpu.VMEM((lookup_count, node_count), jnp.int32),
            pltpu.SemaphoreType.DMA((3,)),
        ],
    )
    flat_ids = swap_all(requests).reshape(-1)
    (fetched,) = call(
        partial(fetch_kernel, min(64, capacity)),
        [on_chip((slot_count, table_width), bf16)],
        [SMEM, CHIP],
        (flat_ids, held),
        scratch=[pltpu.VMEM((LANES, table_width), f32)],
    )
    returned = swap_all(fetched.reshape(devices, capacity, table_width))
    map_pool, map_self, cleared = call(
        prep_kernel,
        [
            in_hbm((table_width, hidden), bf16),
            in_hbm((table_width, hidden), bf16),
            on_chip((rows_local + SPARE, table_width), f32),
        ],
        [CHIP] + [HBM] * 3,
        (fetched, w_in, w_pool, w_self),
        scratch=[
            pltpu.VMEM(w_in.shape, bf16),
            pltpu.VMEM(w_pool.shape, bf16),
            pltpu.VMEM(w_self.shape, bf16),
            pltpu.SemaphoreType.DMA((3,)),
        ],
        flops=10**9,
    )
    (feature,) = call(
        combine_kernel,
        [on_chip((node_count, table_width), bf16)],
        [CHIP, CHIP, HBM],
        (place, returned.reshape(slot_count, table_width), map_pool),
    )
    half = domains // 2
    far = shift(feature, half)
    near = [shift(feature, mask) for mask in range(1, half)]
    pieces = [feature, *near, far, *[shift(far, mask) for mask in range(1, half)]]
    map_pool, adjacency = call(
        warm_kernel,
        [on_chip(map_pool.shape, bf16), on_chip(adjacency.shape, bf16)],
        [CHIP, HBM, HBM],
        (far, map_pool, adjacency),
        scratch=[pltpu.SemaphoreType.DMA((2,))],
        flops=10**8,
    )
    index = ((neighbour_part ^ lax.axis_index("dom")) * block_count + neighbour_block).reshape(-1)
    node_out, d_self, *owed = call(
        partial(sage_kernel, domains),
        [
            in_hbm((node_count, hidden), bf16, HBM),
            in_hbm((node_count, table_width), f32, HBM),
            *[on_chip((node_count, table_width), bf16) for _ in range(domains)],
        ],
        [HBM] + [CHIP] * (domains + 2) + [HBM] * 4,
        (
            index,
            *pieces,
            map_pool,
            adjacency,
            map_self,
            w_neigh,
            out_gain.reshape(1, hidden),
            cotangent,
        ),
        scratch=[
            pltpu.VMEM(map_self.shape, bf16),
            pltpu.VMEM(w_neigh.shape, bf16),
            pltpu.VMEM((1, hidden), bf16),
            pltpu.VMEM(cotangent.shape, bf16),
            pltpu.SemaphoreType.DMA((9,)),
            pltpu.VMEM((node_count, hidden), bf16),
            pltpu.VMEM((node_count, table_width), f32),
            pltpu.SMEM((block_count * fanout,), jnp.int32),
            pltpu.VMEM((domains * block_count, block_rows, table_width), bf16),
            pltpu.VMEM((node_count * fanout, hidden), f32),
            pltpu.VMEM((node_count, hidden), bf16),
            pltpu.VMEM((node_count, LANES), f32),
            pltpu.VMEM((node_count, hidden), f32),
            pltpu.VMEM((node_count, hidden), bf16),
            pltpu.VMEM((node_count, hidden), f32),
            pltpu.VMEM((domains * block_count, block_rows, table_width), f32),
        ],
        flops=5 * 10**9,
    )
    relayed = [shift(owed[half + mask], mask) for mask in range(1, half)]
    back = [shift(owed[mask], mask) for mask in range(1, half)]
    relay = owed[half].astype(f32)
    for piece in relayed:
        relay = relay + piece.astype(f32)
    back = [owed[0], *back, shift(relay.astype(bf16), half)]
    (outgoing,) = call(
        spread_kernel,
        [on_chip((slot_count, table_width), bf16)],
        [CHIP, VMEM] + [CHIP] * len(back),
        (place, d_self, *back),
    )
    owed_rows = swap_all(outgoing.reshape(devices, capacity, table_width))
    _, table_grad = call(
        partial(deposit_kernel, min(16, capacity), min(64, capacity)),
        [
            on_chip((rows_local + SPARE, table_width), f32),
            in_hbm((rows_local, table_width), f32, HBM),
        ],
        [HBM, HBM, CHIP, CHIP],
        (
            flat_ids,
            flat_ids.reshape(chunks, LANES),
            owed_rows.reshape(slot_count, table_width),
            cleared,
        ),
        scratch=[
            pltpu.VMEM((slot_count, table_width), f32),
            pltpu.SMEM((slot_count,), jnp.int32),
            pltpu.VMEM((chunks, LANES), jnp.int32),
            pltpu.SemaphoreType.DMA((3,)),
        ],
        aliases={3: 0},
    )
    return (node_out, table_grad[None])


def solution(mesh):
    both = P(("table", "dom"), None)
    placed = (
        P("table", "dom", None),
        both,
        both,
        both,
        both,
        P(("table", "dom"), None, None, None),
        P(),
        P(),
        P(),
        P(),
        P(),
        both,
    )
    return jax.shard_map(
        body,
        mesh=mesh,
        in_specs=placed,
        out_specs=(both, P("table", "dom", None)),
        check_vma=False,
    )
```

```python
from functools import partial

import jax
import jax.numpy as jnp
from jax import lax
from jax.experimental import pallas as pl
from jax.experimental.pallas import tpu as pltpu
from jax.sharding import PartitionSpec as P

EPSILON = 1e-06
LANES = 128

VMEM = pltpu.VMEM
SMEM = pltpu.SMEM
HBM = pltpu.HBM
CHIP = "chip"
SPARE = 8


def call(kernel, outs, ins_space, args, scratch=(), flops=0, aliases=None):
    args = [
        pltpu.with_memory_space_constraint(arg, VMEM if space == CHIP else HBM)
        if space in (CHIP, HBM)
        else arg
        for space, arg in zip(ins_space, args)
    ]
    return pl.pallas_call(
        kernel,
        out_shape=[out for _, out in outs],
        in_specs=[pl.BlockSpec(memory_space=VMEM if s == CHIP else s) for s in ins_space],
        out_specs=[pl.BlockSpec(memory_space=space) for space, _ in outs],
        scratch_shapes=list(scratch),
        input_output_aliases=aliases or {},
        compiler_params=pltpu.CompilerParams(vmem_limit_bytes=40 << 20),
        cost_estimate=pl.CostEstimate(flops=flops, transcendentals=0, bytes_accessed=1 << 20),
    )(*args)


def on_chip(shape, dtype):
    return VMEM, pltpu.VMEM(shape, dtype)


def in_hbm(shape, dtype, space=VMEM):
    return space, jax.ShapeDtypeStruct(shape, dtype)


def dot(left, right, left_dim, right_dim):
    return lax.dot_general(
        left, right, (((left_dim,), (right_dim,)), ((), ())), preferred_element_type=jnp.float32
    )


def ones_where(mask):
    return jnp.where(mask, 1.0, 0.0).astype(jnp.bfloat16)


def silu_parts(half):
    upper = jnp.tanh(half) + 1.0
    value = half * upper
    return value, upper + value * (2.0 - upper)


def route_kernel(
    owner_in, row_in, table_ref, request_ref, place_ref, held_ref, owner_ref, row_ref, sems
):
    owner_load = pltpu.make_async_copy(owner_in, owner_ref, sems.at[0])
    row_load = pltpu.make_async_copy(row_in, row_ref, sems.at[1])
    load = pltpu.make_async_copy(
        table_ref, held_ref.at[pl.ds(SPARE, table_ref.shape[0]), :], sems.at[2]
    )
    owner_load.start()
    row_load.start()
    load.start()
    held_ref[:SPARE, :] = jnp.zeros((SPARE, held_ref.shape[1]), jnp.float32)
    lookups, nodes = owner_ref.shape
    devices, capacity = request_ref.shape
    owners = lax.broadcasted_iota(jnp.int32, (devices, nodes), 0)
    earlier = ones_where(
        lax.broadcasted_iota(jnp.int32, (nodes, nodes), 0)
        < lax.broadcasted_iota(jnp.int32, (nodes, nodes), 1)
    )
    owner_load.wait()
    row_load.wait()
    hits = [owner_ref[j : j + 1, :] == owners for j in range(lookups)]
    before = dot(jnp.concatenate([ones_where(hit) for hit in hits], axis=0), earlier, 1, 0)
    carry = jnp.zeros((devices, 1), jnp.float32)
    place = jnp.zeros((devices, nodes), jnp.float32)
    slots = lax.broadcasted_iota(jnp.int32, (capacity, nodes), 0).astype(jnp.float32)
    high, low, taken = [], [], []
    for j in range(lookups):
        position = before[j * devices : (j + 1) * devices, :] + carry
        carry = carry + jnp.sum(jnp.where(hits[j], 1.0, 0.0), axis=1, keepdims=True)
        place = place + jnp.where(hits[j], position + 1.0, 0.0)
        own = jnp.sum(jnp.where(hits[j], position, 0.0), axis=0, keepdims=True)
        taken.append(ones_where(own == slots))
        row = row_ref[j : j + 1, :] + 1
        upper = (row >> 7).astype(jnp.float32)
        lower = (row & 127).astype(jnp.float32)
        high.append(jnp.where(hits[j], upper, 0.0).astype(jnp.bfloat16))
        low.append(jnp.where(hits[j], lower, 0.0).astype(jnp.bfloat16))
    taken = jnp.concatenate(taken, axis=1)
    request = dot(jnp.concatenate(high, axis=1), taken, 1, 1) * 128.0 + dot(
        jnp.concatenate(low, axis=1), taken, 1, 1
    )
    request_ref[...] = request.astype(jnp.int32)
    place_ref[...] = place.astype(jnp.int32) - 1
    load.wait()


def prep_kernel(
    _,
    w_in_ref,
    w_pool_ref,
    w_self_ref,
    map_pool_ref,
    map_self_ref,
    sums_ref,
    w_in_held,
    w_pool_held,
    w_self_held,
    sems,
):
    copies = [
        pltpu.make_async_copy(source, target, sems.at[i])
        for i, (source, target) in enumerate(
            [(w_in_ref, w_in_held), (w_pool_ref, w_pool_held), (w_self_ref, w_self_held)]
        )
    ]
    for copy in copies:
        copy.start()

    def clear(i, _):
        start = pl.multiple_of(i * 64, 64)
        sums_ref[pl.ds(start, 64), :] = jnp.zeros((64, sums_ref.shape[1]), jnp.float32)
        return 0

    whole = sums_ref.shape[0] // 64
    lax.fori_loop(0, whole, clear, 0)
    rest = sums_ref.shape[0] - whole * 64
    if rest:
        sums_ref[whole * 64 :, :] = jnp.zeros((rest, sums_ref.shape[1]), jnp.float32)
    copies[0].wait()
    copies[1].wait()
    map_pool_ref[...] = (0.5 * dot(w_in_held[...], w_pool_held[...], 1, 0)).astype(jnp.bfloat16)
    copies[2].wait()
    map_self_ref[...] = (0.5 * dot(w_in_held[...], w_self_held[...], 1, 0)).astype(jnp.bfloat16)


def warm_kernel(_, pool_in, adjacency_in, pool_out, adjacency_out, sems):
    loads = [
        pltpu.make_async_copy(pool_in, pool_out, sems.at[0]),
        pltpu.make_async_copy(adjacency_in, adjacency_out, sems.at[1]),
    ]
    for load in loads:
        load.start()
    for load in loads:
        load.wait()


def fetch_kernel(size, id_ref, table_ref, out_ref, rows_ref):
    chunks = out_ref.shape[0] // LANES
    rows_ref[...] = jnp.zeros(rows_ref.shape, jnp.float32)

    def step(chunk, _):
        for group in range(LANES // size):
            base = chunk * LANES + group * size

            @pl.when(id_ref[base] > 0)
            def _():
                for i in range(size):
                    row = id_ref[base + i] + (SPARE - 1)
                    rows_ref[pl.ds(group * size + i, 1), :] = table_ref[pl.ds(row, 1), :]

        start = pl.multiple_of(chunk * LANES, LANES)
        out_ref[pl.ds(start, LANES), :] = rows_ref[...].astype(jnp.bfloat16)
        return 0

    lax.fori_loop(0, chunks, step, 0)


def select_rows(place_ref, first, count, capacity):
    nodes = place_ref.shape[1]
    slots = lax.broadcasted_iota(jnp.int32, (capacity, nodes), 0)
    parts = [ones_where(place_ref[o : o + 1, :] == slots) for o in range(first, first + count)]
    return jnp.concatenate(parts, axis=0)


def combine_kernel(place_ref, returned_ref, _, feature_ref):
    devices = place_ref.shape[0]
    capacity = returned_ref.shape[0] // devices
    count = max(1, 512 // capacity)
    total = None
    for first in range(0, devices, count):
        chosen = select_rows(place_ref, first, count, capacity)
        rows = returned_ref[first * capacity : (first + count) * capacity, :]
        part = dot(rows, chosen, 0, 0)
        total = part if total is None else total + part
    feature_ref[...] = total.T.astype(jnp.bfloat16)


def spread_kernel(place_ref, d_self_ref, *refs):
    *back_refs, out_ref = refs
    devices = place_ref.shape[0]
    capacity = out_ref.shape[0] // devices
    count = max(1, 512 // capacity)
    total = d_self_ref[...]
    for back_ref in back_refs:
        total = total + back_ref[...].astype(jnp.float32)
    d_feature = total.astype(jnp.bfloat16)
    for first in range(0, devices, count):
        chosen = select_rows(place_ref, first, count, capacity)
        out_ref[first * capacity : (first + count) * capacity, :] = dot(
            chosen, d_feature, 1, 0
        ).astype(jnp.bfloat16)


def deposit_kernel(
    size, gate, flat_in, ids_in, grad_ref, _, sums_ref, out_ref, fresh_ref, id_ref, ids_ref, sems
):
    chunks = ids_ref.shape[0]
    load_ids = pltpu.make_async_copy(ids_in, ids_ref, sems.at[1])
    load = pltpu.make_async_copy(flat_in, id_ref, sems.at[2])
    load_ids.start()
    load.start()
    load_ids.wait()
    rows = ids_ref[...].astype(jnp.float32)
    columns = rows.T
    same_group = (
        lax.broadcasted_iota(jnp.int32, (LANES, LANES), 0) // size
        == lax.broadcasted_iota(jnp.int32, (LANES, LANES), 1) // size
    )
    for chunk in range(chunks):
        same = (columns[:, chunk : chunk + 1] == rows[chunk : chunk + 1, :]) & same_group
        fresh_ref[chunk * LANES : (chunk + 1) * LANES, :] = dot(
            ones_where(same), grad_ref[chunk * LANES : (chunk + 1) * LANES, :], 1, 0
        )

    def step(chunk, _):
        for part in range(LANES // gate):
            first = chunk * LANES + part * gate

            @pl.when(id_ref[first] > 0)
            def _():
                for group in range(gate // size):
                    base = first + group * size
                    targets = [id_ref[base + i] + (SPARE - 1) for i in range(size)]
                    fresh = [
                        sums_ref[pl.ds(targets[i], 1), :] + fresh_ref[pl.ds(base + i, 1), :]
                        for i in range(size)
                    ]
                    for i in range(size):
                        sums_ref[pl.ds(targets[i], 1), :] = fresh[i]

        return 0

    load.wait()
    lax.fori_loop(0, chunks, step, 0)
    store = pltpu.make_async_copy(sums_ref.at[pl.ds(SPARE, out_ref.shape[0]), :], out_ref, sems.at[0])
    store.start()
    store.wait()


def sage_kernel(domains, *refs):
    index_in, *piece_refs = refs[: domains + 1]
    map_pool_ref, adjacency_ref, *in_refs = refs[domains + 1 : domains + 7]
    node_out_ref, d_self_ref, *owed_refs = refs[domains + 7 : 2 * domains + 9]
    (
        map_self_ref,
        w_neigh_ref,
        gain_ref,
        cotangent_ref,
        sems,
        result_ref,
        d_self_held,
        index_ref,
        gathered_ref,
        slope_ref,
        mean_ref,
        inverse_ref,
        pre_ref,
        d_pre_ref,
        d_mean_ref,
        total_ref,
    ) = refs[2 * domains + 9 :]
    blocks, fanout, block_rows, _ = adjacency_ref.shape
    held = [map_self_ref, w_neigh_ref, gain_ref, cotangent_ref]
    loads = [
        pltpu.make_async_copy(source, target, sems.at[i])
        for i, (source, target) in enumerate(zip(in_refs, held))
    ]
    load_index = pltpu.make_async_copy(index_in, index_ref, sems.at[len(loads) + 2])
    load_index.start()
    for load in loads:
        load.start()
    for mask in range(domains):
        for block in range(blocks):
            gathered_ref[mask * blocks + block] = piece_refs[mask][
                block * block_rows : (block + 1) * block_rows, :
            ]
    nodes, hidden = pre_ref.shape
    span = fanout * block_rows

    def wide(block):
        return jnp.concatenate([adjacency_ref[block, k] for k in range(fanout)], axis=1)

    def forward(block, _):
        sources = jnp.concatenate(
            [gathered_ref[index_ref[block * fanout + k]] for k in range(fanout)], axis=0
        )
        start = pl.multiple_of(block * span, span)
        pooled, slope_ref[pl.ds(start, span), :] = silu_parts(dot(sources, map_pool_ref[...], 1, 0))
        pooled = pooled.astype(jnp.bfloat16)
        weights = wide(block)
        inverse = 1.0 / jnp.sum(weights.astype(jnp.float32), axis=1, keepdims=True)
        own = pl.multiple_of(block * block_rows, block_rows)
        inverse_ref[pl.ds(own, block_rows), :] = jnp.broadcast_to(inverse, (block_rows, LANES))
        mean_ref[pl.ds(own, block_rows), :] = (dot(weights, pooled, 1, 0) * (0.5 * inverse)).astype(
            jnp.bfloat16
        )
        return 0

    load_index.wait()
    lax.fori_loop(0, blocks, forward, 0, unroll=2)
    for load in loads:
        load.wait()
    pre_ref[...] = dot(piece_refs[0][...], map_self_ref[...], 1, 0) + dot(
        mean_ref[...], w_neigh_ref[...], 1, 0
    )
    gain = gain_ref[...].astype(jnp.float32)
    piece = 128

    def middle(part, _):
        start = pl.multiple_of(part * piece, piece)
        here = pl.ds(start, piece)
        active, slope = silu_parts(pre_ref[here, :])
        scale = lax.rsqrt(jnp.mean(active * active, axis=1, keepdims=True) + EPSILON)
        result_ref[here, :] = (active * scale * gain).astype(jnp.bfloat16)
        weighted = gain * cotangent_ref[here, :].astype(jnp.float32)
        shift = (scale * scale * scale) * jnp.mean(weighted * active, axis=1, keepdims=True)
        half_d_active = (0.5 * scale) * weighted - active * (0.5 * shift)
        d_pre_ref[here, :] = (half_d_active * slope).astype(jnp.bfloat16)
        return 0

    lax.fori_loop(0, nodes // piece, middle, 0)
    store = pltpu.make_async_copy(result_ref, node_out_ref, sems.at[len(loads)])
    store.start()
    d_pre = d_pre_ref[...]
    d_self_held[...] = 2.0 * dot(d_pre, map_self_ref[...], 1, 1)
    store_self = pltpu.make_async_copy(d_self_held, d_self_ref, sems.at[len(loads) + 1])
    store_self.start()
    d_mean_ref[...] = dot(d_pre, w_neigh_ref[...], 1, 1)
    total_ref[...] = jnp.zeros(total_ref.shape, jnp.float32)

    def backward(block, _):
        own = pl.multiple_of(block * block_rows, block_rows)
        inverse = inverse_ref[pl.ds(own, block_rows), :][:, :1]
        d_scaled = (d_mean_ref[pl.ds(own, block_rows), :] * inverse).astype(jnp.bfloat16)
        start = pl.multiple_of(block * span, span)
        share = dot(wide(block), d_scaled, 0, 0)
        d_pool = (share * slope_ref[pl.ds(start, span), :]).astype(jnp.bfloat16)
        d_source = dot(d_pool, map_pool_ref[...], 1, 1)
        for k in range(fanout):
            target = index_ref[block * fanout + k]
            total_ref[target] += d_source[k * block_rows : (k + 1) * block_rows, :]
        return 0

    lax.fori_loop(0, blocks, backward, 0, unroll=2)
    for mask in range(domains):
        for block in range(blocks):
            owed_refs[mask][block * block_rows : (block + 1) * block_rows, :] = total_ref[
                mask * blocks + block
            ].astype(jnp.bfloat16)
    store.wait()
    store_self.wait()


def shift(piece, mask):
    domains = lax.axis_size("dom")
    return lax.ppermute(piece, "dom", [(i, i ^ mask) for i in range(domains)])


def swap_all(buffer):
    return lax.all_to_all(buffer, ("table", "dom"), split_axis=0, concat_axis=0, tiled=True)


def body(
    tables,
    owner_ids,
    row_ids,
    neighbour_part,
    neighbour_block,
    adjacency,
    w_in,
    w_pool,
    w_self,
    w_neigh,
    out_gain,
    cotangent,
):
    groups = lax.axis_size("table")
    domains = lax.axis_size("dom")
    devices = groups * domains
    node_count, lookup_count = owner_ids.shape
    table_width = tables.shape[2]
    rows_local = tables.shape[1]
    hidden = w_self.shape[0]
    block_rows = adjacency.shape[-1]
    block_count = node_count // block_rows
    fanout = neighbour_part.shape[1]
    capacity = max(2, (2 * node_count * lookup_count + devices - 1) // devices)
    slot_count = devices * capacity
    chunks = slot_count // LANES
    f32, bf16 = jnp.float32, jnp.bfloat16

    requests, place, held = call(
        route_kernel,
        [
            on_chip((devices, capacity), jnp.int32),
            on_chip((devices, node_count), jnp.int32),
            on_chip((rows_local + SPARE, table_width), f32),
        ],
        [HBM, HBM, HBM],
        (owner_ids.T, row_ids.T, tables[0]),
        scratch=[
            pltpu.VMEM((lookup_count, node_count), jnp.int32),
            pltpu.VMEM((lookup_count, node_count), jnp.int32),
            pltpu.SemaphoreType.DMA((3,)),
        ],
    )
    flat_ids = swap_all(requests).reshape(-1)
    (fetched,) = call(
        partial(fetch_kernel, min(128, capacity)),
        [on_chip((slot_count, table_width), bf16)],
        [SMEM, CHIP],
        (flat_ids, held),
        scratch=[pltpu.VMEM((LANES, table_width), f32)],
    )
    returned = swap_all(fetched.reshape(devices, capacity, table_width))
    map_pool, map_self, cleared = call(
        prep_kernel,
        [
            in_hbm((table_width, hidden), bf16),
            in_hbm((table_width, hidden), bf16),
            on_chip((rows_local + SPARE, table_width), f32),
        ],
        [CHIP] + [HBM] * 3,
        (fetched, w_in, w_pool, w_self),
        scratch=[
            pltpu.VMEM(w_in.shape, bf16),
            pltpu.VMEM(w_pool.shape, bf16),
            pltpu.VMEM(w_self.shape, bf16),
            pltpu.SemaphoreType.DMA((3,)),
        ],
        flops=10**9,
    )
    (feature,) = call(
        combine_kernel,
        [on_chip((node_count, table_width), bf16)],
        [CHIP, CHIP, HBM],
        (place, returned.reshape(slot_count, table_width), map_pool),
    )
    half = domains // 2
    far = shift(feature, half)
    near = [shift(feature, mask) for mask in range(1, half)]
    pieces = [feature, *near, far, *[shift(far, mask) for mask in range(1, half)]]
    map_pool, adjacency = call(
        warm_kernel,
        [on_chip(map_pool.shape, bf16), on_chip(adjacency.shape, bf16)],
        [CHIP, HBM, HBM],
        (far, map_pool, adjacency),
        scratch=[pltpu.SemaphoreType.DMA((2,))],
        flops=10**8,
    )
    index = ((neighbour_part ^ lax.axis_index("dom")) * block_count + neighbour_block).reshape(-1)
    node_out, d_self, *owed = call(
        partial(sage_kernel, domains),
        [
            in_hbm((node_count, hidden), bf16, HBM),
            in_hbm((node_count, table_width), f32, HBM),
            *[on_chip((node_count, table_width), bf16) for _ in range(domains)],
        ],
        [HBM] + [CHIP] * (domains + 2) + [HBM] * 4,
        (
            index,
            *pieces,
            map_pool,
            adjacency,
            map_self,
            w_neigh,
            out_gain.reshape(1, hidden),
            cotangent,
        ),
        scratch=[
            pltpu.VMEM(map_self.shape, bf16),
            pltpu.VMEM(w_neigh.shape, bf16),
            pltpu.VMEM((1, hidden), bf16),
            pltpu.VMEM(cotangent.shape, bf16),
            pltpu.SemaphoreType.DMA((9,)),
            pltpu.VMEM((node_count, hidden), bf16),
            pltpu.VMEM((node_count, table_width), f32),
            pltpu.SMEM((block_count * fanout,), jnp.int32),
            pltpu.VMEM((domains * block_count, block_rows, table_width), bf16),
            pltpu.VMEM((node_count * fanout, hidden), f32),
            pltpu.VMEM((node_count, hidden), bf16),
            pltpu.VMEM((node_count, LANES), f32),
            pltpu.VMEM((node_count, hidden), f32),
            pltpu.VMEM((node_count, hidden), bf16),
            pltpu.VMEM((node_count, hidden), f32),
            pltpu.VMEM((domains * block_count, block_rows, table_width), f32),
        ],
        flops=5 * 10**9,
    )
    relayed = [shift(owed[half + mask], mask) for mask in range(1, half)]
    back = [shift(owed[mask], mask) for mask in range(1, half)]
    relay = owed[half].astype(f32)
    for piece in relayed:
        relay = relay + piece.astype(f32)
    back = [owed[0], *back, shift(relay.astype(bf16), half)]
    (outgoing,) = call(
        spread_kernel,
        [on_chip((slot_count, table_width), bf16)],
        [CHIP, VMEM] + [CHIP] * len(back),
        (place, d_self, *back),
    )
    owed_rows = swap_all(outgoing.reshape(devices, capacity, table_width))
    _, table_grad = call(
        partial(deposit_kernel, min(16, capacity), min(64, capacity)),
        [
            on_chip((rows_local + SPARE, table_width), f32),
            in_hbm((rows_local, table_width), f32, HBM),
        ],
        [HBM, HBM, CHIP, CHIP],
        (
            flat_ids,
            flat_ids.reshape(chunks, LANES),
            owed_rows.reshape(slot_count, table_width),
            cleared,
        ),
        scratch=[
            pltpu.VMEM((slot_count, table_width), f32),
            pltpu.SMEM((slot_count,), jnp.int32),
            pltpu.VMEM((chunks, LANES), jnp.int32),
            pltpu.SemaphoreType.DMA((3,)),
        ],
        aliases={3: 0},
    )
    return (node_out, table_grad[None])


def solution(mesh):
    both = P(("table", "dom"), None)
    placed = (
        P("table", "dom", None),
        both,
        both,
        both,
        both,
        P(("table", "dom"), None, None, None),
        P(),
        P(),
        P(),
        P(),
        P(),
        both,
    )
    return jax.shard_map(
        body,
        mesh=mesh,
        in_specs=placed,
        out_specs=(both, P("table", "dom", None)),
        check_vma=False,
    )
```
